32 devices in a mesh: dp: 4 (over y, z), tp: 8 (over x, core).
Axes of the slice: x: 4, y: 2, z: 2, core: 2. Of those that a mesh axis runs over, the one named last changes fastest.
The devices are a block of a 4x4x8 slice.
Arguments:
- x_in: bfloat16 [4, 3072, 3584], P('dp', 'tp'), parts along dimension 0
- positions: int32 [4, 3072], P('dp', 'tp'), parts along dimension 0
- grad_out: bfloat16 [4, 3072, 3584], P('dp', 'tp'), parts along dimension 0
- w_query: bfloat16 [3584, 16, 256], P(None, 'tp')
- w_key: bfloat16 [3584, 8, 256], P(None, 'tp')
- w_value: bfloat16 [3584, 8, 256], P(None, 'tp')
- w_out: bfloat16 [16, 256, 3584], P('tp')
- gain_pre: float32 [3584], replicated
- gain_post: float32 [3584], replicated
Outputs:
- output 1: bfloat16 [4, 3072, 3584], P('dp', 'tp'), parts along dimension 0
- output 2: bfloat16 [4, 3072, 3584], P('dp', 'tp'), parts along dimension 0
- output 3: float32 [14336, 16, 256], P('dp', 'tp'), parts along dimension 0
- output 4: float32 [14336, 8, 256], P('dp', 'tp'), parts along dimension 0
- output 5: float32 [14336, 8, 256], P('dp', 'tp'), parts along dimension 0
- output 6: float32 [64, 256, 3584], P(('dp', 'tp')), parts along dimension 0
- output 7: float32 [14336], P('dp'), parts along dimension 0
- output 8: float32 [14336], P('dp'), parts along dimension 0
There are 4 independent parts. The reference program is written for one: setup_inputs(seed, part) draws one part's arguments, and reference() takes and returns one part's arrays. A program takes and returns all parts, laid end to end along the dimension named above; an argument that names none is the same for every part.
All inputs are finite; a program needn't handle non-finite values.
Results may differ from the reference program's by a relative error of at most 0.0190464.
Values are sent between devices in bfloat16 or wider.
A program may use at most 768 MiB of HBM per device.

```python
import functools
import jax
import jax.numpy as jnp
from jax import lax

BATCH_ROWS = 1
SEQ_LEN = 3072
MODEL_DIM = 3584
NUM_HEADS = 16
KV_HEADS = 8
HEAD_DIM = 256
WINDOW = 4096
QUERY_BLOCK = 128
SOFT_CAP = 50.0
NORM_EPS = 1e-6
ROPE_THETA = 10000.0


def draw_positions(pos_key, n_rows, seq_len):
    key_off, key_hit, key_jump = jax.random.split(pos_key, 3)
    offset = jax.random.randint(key_off, (n_rows, 1), 0, WINDOW)
    hit_draw = jax.random.randint(key_hit, (n_rows, seq_len), 0, max(seq_len // 8, 1))
    jump_size = jax.random.randint(key_jump, (n_rows, seq_len), 1, 2 * WINDOW)
    pos_steps = 1 + jnp.where(hit_draw == 0, jump_size, 0)
    return (offset + jnp.cumsum(pos_steps, axis=1) - pos_steps[:, :1]).astype(jnp.int32)


def setup_inputs(seed: int = 0, part: int = 0) -> dict:
    base_key = jax.random.key(seed)
    part_key = jax.random.fold_in(base_key, part)
    key_x, key_pos, key_dy = jax.random.split(part_key, 3)
    key_q, key_k, key_v, key_o, key_gp, key_gq = jax.random.split(base_key, 6)
    act_shape = (BATCH_ROWS, SEQ_LEN, MODEL_DIM)
    in_scale = MODEL_DIM ** -0.5
    out_scale = (NUM_HEADS * HEAD_DIM) ** -0.5
    x_in = jax.random.normal(key_x, act_shape, jnp.float32).astype(jnp.bfloat16)
    positions = draw_positions(key_pos, BATCH_ROWS, SEQ_LEN)
    grad_out = jax.random.normal(key_dy, act_shape, jnp.float32).astype(jnp.bfloat16)
    w_query = (jax.random.normal(key_q, (MODEL_DIM, NUM_HEADS, HEAD_DIM), jnp.float32) * in_scale).astype(jnp.bfloat16)
    w_key = (jax.random.normal(key_k, (MODEL_DIM, KV_HEADS, HEAD_DIM), jnp.float32) * in_scale).astype(jnp.bfloat16)
    w_value = (jax.random.normal(key_v, (MODEL_DIM, KV_HEADS, HEAD_DIM), jnp.float32) * in_scale).astype(jnp.bfloat16)
    w_out = (jax.random.normal(key_o, (NUM_HEADS, HEAD_DIM, MODEL_DIM), jnp.float32) * out_scale).astype(jnp.bfloat16)
    gain_pre = 0.5 * jax.random.normal(key_gp, (MODEL_DIM,), jnp.float32)
    gain_post = 0.5 * jax.random.normal(key_gq, (MODEL_DIM,), jnp.float32)
    return {'x_in': x_in, 'positions': positions, 'grad_out': grad_out, 'w_query': w_query, 'w_key': w_key, 'w_value': w_value, 'w_out': w_out, 'gain_pre': gain_pre, 'gain_post': gain_post}


def rms_norm(hidden, scale_w):
    values = hidden.astype(jnp.float32)
    inv_rms = lax.rsqrt(jnp.mean(values * values, axis=-1, keepdims=True) + NORM_EPS)
    return (values * inv_rms * (1.0 + scale_w)).astype(jnp.bfloat16)


def rope_tables(positions, head_dim):
    half_dim = head_dim // 2
    inv_freq = ROPE_THETA ** (-2.0 * jnp.arange(half_dim, dtype=jnp.float32) / head_dim)
    angles = positions.astype(jnp.float32)[:, :, None] * inv_freq
    return jnp.cos(angles)[:, :, None, :], jnp.sin(angles)[:, :, None, :]


def apply_rope(values, cos_t, sin_t):
    half_dim = values.shape[-1] // 2
    lo_half = values[..., :half_dim]
    hi_half = values[..., half_dim:]
    return jnp.concatenate([lo_half * cos_t - hi_half * sin_t, hi_half * cos_t + lo_half * sin_t], axis=-1)


def block_probs(q_blk, k_blk, pos_q, pos_k):
    scores = jnp.einsum('bqkgd,bskd->bkgqs', q_blk.astype(jnp.float32), k_blk.astype(jnp.float32))
    capped = SOFT_CAP * jnp.tanh(scores / SOFT_CAP)
    pos_gap = pos_q[:, :, None] - pos_k[:, None, :]
    in_window = ((pos_gap >= 0) & (pos_gap < WINDOW))[:, None, None, :, :]
    return jax.nn.softmax(jnp.where(in_window, capped, -1e30), axis=-1)


def attention(q_all, k_all, v_all, positions):
    seq_len = positions.shape[1]
    q_block = min(QUERY_BLOCK, seq_len)
    slab_len = min(WINDOW + q_block, seq_len)

    def one_block(blk_idx):
        q_start = blk_idx * q_block
        k_start = jnp.maximum(q_start + q_block - slab_len, 0)
        q_blk = lax.dynamic_slice_in_dim(q_all, q_start, q_block, axis=1)
        k_blk = lax.dynamic_slice_in_dim(k_all, k_start, slab_len, axis=1)
        v_blk = lax.dynamic_slice_in_dim(v_all, k_start, slab_len, axis=1)
        pos_q = lax.dynamic_slice_in_dim(positions, q_start, q_block, axis=1)
        pos_k = lax.dynamic_slice_in_dim(positions, k_start, slab_len, axis=1)
        prob_blk = block_probs(q_blk, k_blk, pos_q, pos_k)
        out_blk = jnp.einsum('bkgqs,bskd->bqkgd', prob_blk.astype(jnp.bfloat16).astype(jnp.float32), v_blk.astype(jnp.float32))
        return out_blk.astype(jnp.bfloat16)

    blocks = lax.map(jax.checkpoint(one_block), jnp.arange(seq_len // q_block))
    return jnp.moveaxis(blocks, 0, 1).reshape(q_all.shape)


def forward(positions, x_in, w_query, w_key, w_value, w_out, gain_pre, gain_post):
    n_rows, seq_len = positions.shape
    num_heads, head_dim = w_query.shape[1], w_query.shape[2]
    kv_heads = w_key.shape[1]
    normed = rms_norm(x_in, gain_pre).astype(jnp.float32)
    cos_t, sin_t = rope_tables(positions, head_dim)
    q_lin = jnp.einsum('bsd,dhe->bshe', normed, w_query.astype(jnp.float32))
    k_lin = jnp.einsum('bsd,dhe->bshe', normed, w_key.astype(jnp.float32))
    v_lin = jnp.einsum('bsd,dhe->bshe', normed, w_value.astype(jnp.float32))
    q_all = (apply_rope(q_lin, cos_t, sin_t) * head_dim ** -0.5).astype(jnp.bfloat16)
    q_all = q_all.reshape(n_rows, seq_len, kv_heads, num_heads // kv_heads, head_dim)
    k_all = apply_rope(k_lin, cos_t, sin_t).astype(jnp.bfloat16)
    v_all = v_lin.astype(jnp.bfloat16)
    attn_out = attention(q_all, k_all, v_all, positions).reshape(n_rows, seq_len, num_heads, head_dim)
    proj_out = jnp.einsum('bshe,hed->bsd', attn_out.astype(jnp.float32), w_out.astype(jnp.float32)).astype(jnp.bfloat16)
    post_norm = rms_norm(proj_out, gain_post)
    return (x_in.astype(jnp.float32) + post_norm.astype(jnp.float32)).astype(jnp.bfloat16)


def reference(x_in, positions, grad_out, w_query, w_key, w_value, w_out, gain_pre, gain_post):
    y_out, pullback = jax.vjp(functools.partial(forward, positions), x_in, w_query, w_key, w_value, w_out, gain_pre, gain_post)
    grad_x, grad_wq, grad_wk, grad_wv, grad_wo, grad_pre, grad_post = pullback(grad_out)
    return (y_out, grad_x, grad_wq.astype(jnp.float32), grad_wk.astype(jnp.float32), grad_wv.astype(jnp.float32), grad_wo.astype(jnp.float32), grad_pre.astype(jnp.float32), grad_post.astype(jnp.float32))
```

```python
import functools

import jax
import jax.numpy as jnp
import numpy as np
from jax import lax
from jax.experimental import pallas as pl
from jax.experimental.pallas import tpu as pltpu
from jax.sharding import PartitionSpec as P


WINDOW = 4096
SOFT_CAP = 50.0
NORM_EPS = 1e-6
ROPE_THETA = 10000.0
LOG2E = 1.4426950408889634
BLK = 128
PIECE = 64
SUB = 16
KT = 512
NBLK = 3
NPC = 6
HALF_PC = 3
CHIPS = 4
DEVS = 8
ALL_BLK = DEVS * NBLK
MY_BLK = CHIPS * NBLK
HD = 256
HD2 = 128
QW = 512
QKV = 1024
ONE, TWO = 1, 2
VMEM_BYTES = 67 * 1000 * 1000
F32 = jnp.float32
BF16 = jnp.bfloat16
I32 = jnp.int32


def dot(a, b):
    return lax.dot_general(a, b, (((1,), (0,)), ((), ())), preferred_element_type=F32)


def dot_bt(a, b):
    return lax.dot_general(a, b, (((1,), (1,)), ((), ())), preferred_element_type=F32)


def dot_at(a, b):
    return lax.dot_general(a, b, (((0,), (0,)), ((), ())), preferred_element_type=F32)


def pick(s, values):
    out = I32(values[0])
    for i, value in enumerate(values):
        if value != values[0]:
            out = jnp.where(s == i, I32(value), out)
    return out


def rcopy(src, dst, ss, rs, dev):
    return pltpu.make_async_remote_copy(src_ref=src, dst_ref=dst, send_sem=ss, recv_sem=rs,
                                        device_id={'tp': dev}, device_id_type=pl.DeviceIdType.MESH)


class Place:
    def __init__(self):
        me = lax.axis_index('tp')
        self.me = me
        self.chip = lax.div(me, TWO)
        self.core = lax.rem(me, TWO)
        self.right = self.dev(ONE, 0)
        self.left = self.dev(CHIPS - ONE, 0)
        self.partner = self.dev(0, ONE)

    def dev(self, chip_off, flip):
        chip = lax.rem(self.chip + chip_off, CHIPS)
        return TWO * chip + lax.rem(self.core + flip, TWO)

    def peers(self):
        return [lax.rem(self.me + d, DEVS) for d in range(ONE, DEVS)]


def barrier(devs):
    sem = pltpu.get_barrier_semaphore()
    for dev in devs:
        pl.semaphore_signal(sem, inc=ONE, device_id={'tp': dev}, device_id_type=pl.DeviceIdType.MESH)
    pl.semaphore_wait(sem, len(devs))


def rows16(r):
    return pl.ds(SUB * r, SUB)


def digits(text):
    return [int(c) for c in text]


AG_OFF = (digits('003033322332'), digits('001011122112'))
AG_FLIP = (digits('000110101010'), digits('010110101011'))
AG_BLK = (digits('020101100221'), digits('102221122001'))
AG_STEPS = len(AG_OFF[0])
AG_FORWARD = {2: ('01', '54'), 5: ('2', '3')}
AG_FIRST = ('0123', '5432')
AG_THEN = ('45', '10')
AG_MADE = digits('051432')
AG_THEN_STEP = 2


def ag_scratch(width):
    dma = pltpu.SemaphoreType.DMA
    return [pltpu.VMEM((ALL_BLK, BLK, width), BF16),
            dma((CHIPS, NPC)),
            dma((CHIPS, NBLK)),
            dma((TWO, NPC)),
            dma((NPC,)),
            dma((CHIPS, NBLK))]


def half_of(i):
    return pl.ds(PIECE * (i % TWO), PIECE)


def piece_of(full, shard, i):
    return full.at[shard * NBLK + i // TWO, half_of(i), :]


def ag_send(p, way, i, src, full, ring_rs, part_rs, own_ss, fwd_ss, part_ss):
    rcopy(src, piece_of(full, p.me, i), own_ss.at[way, i], ring_rs.at[p.chip, i], (p.right, p.left)[way]).start()


def ag_then(s, src):
    @pl.when(s == AG_THEN_STEP)
    def _():
        for way, pieces in enumerate(AG_THEN):
            for i in digits(pieces):
                src(way, i)


def ag_swap(p, chip, blk, src, dst, full, ring_rs, part_rs, own_ss, fwd_ss, part_ss):
    return rcopy(src, dst, part_ss.at[chip, blk], part_rs.at[chip, blk], p.partner)


def ag_block(p, s, n):
    off, flip, blk = pick(s, AG_OFF[n]), pick(s, AG_FLIP[n]), pick(s, AG_BLK[n])
    chip = lax.rem(p.chip + off, CHIPS)
    shard = TWO * chip + lax.rem(p.core + flip, TWO)
    return off, flip, chip, shard, blk, shard * NBLK + blk


def ag_step(p, s, n, full, ring_rs, part_rs, own_ss, fwd_ss, part_ss):
    off, flip, chip, shard, blk, g = ag_block(p, s, n)
    swap = rcopy(full.at[g], full.at[g], part_ss.at[chip, blk], part_rs.at[chip, blk], p.partner)

    @pl.when(flip != 0)
    def _():
        swap.wait_recv()

    @pl.when(jnp.logical_and(flip == 0, off != 0))
    def _():
        for h in range(TWO):
            half = full.at[g, half_of(h), :]
            rcopy(half, half, fwd_ss.at[0], ring_rs.at[chip, TWO * blk + h], p.partner).wait_recv()
        swap.start()

    for step, pieces in AG_FORWARD.items():
        @pl.when(s == step)
        def _(pieces=pieces[n]):
            for i in digits(pieces):
                ref = piece_of(full, shard, i)
                rcopy(ref, ref, fwd_ss.at[i], ring_rs.at[chip, i], (p.right, p.left)[n]).start()
    return g


def ag_finish(p, full, ring_rs, part_rs, own_ss, fwd_ss, part_ss):
    for n in range(NPC):
        ref = piece_of(full, p.me, n)
        for sem in (own_ss.at[0, n], own_ss.at[ONE, n], fwd_ss.at[n]):
            rcopy(ref, ref, sem, ring_rs.at[p.chip, n], p.right).wait_send()
    for c in range(CHIPS):
        for b in range(NBLK):
            ref = full.at[b]
            rcopy(ref, ref, part_ss.at[c, b], part_rs.at[c, b], p.partner).wait_send()


RS_PLAN = ['O23', 'O01', 'O54', 'R54', 'L01', 'X01', 'X23', 'X45', 'R01', 'L54', 'R32', 'L23']


def plan_tables(plan):
    return ([{'O': TWO, 'R': ONE, 'L': CHIPS - ONE, 'X': 0}[step[0]] for step in plan],
            [int(step[ONE]) // TWO for step in plan])


RS_OFF, RS_BLK = plan_tables(RS_PLAN)
RS_STEPS = len(RS_PLAN)
RS_DONE = digits('021')


def rs_scratch(width):
    dma = pltpu.SemaphoreType.DMA
    return [pltpu.VMEM((HALF_PC, NPC, PIECE, width), BF16),
            pltpu.VMEM((HALF_PC, PIECE, width), BF16),
            pltpu.VMEM((HALF_PC, PIECE, width), BF16),
            pltpu.VMEM((TWO, NPC, PIECE, width), BF16),
            pltpu.VMEM((NBLK, BLK, width), BF16),
            dma((HALF_PC, NPC)), dma((HALF_PC,)), dma((HALF_PC,)), dma((TWO, NPC))]


def put_rows(part, dst, i, extra=None):
    @pl.loop(0, PIECE // SUB)
    def _(r):
        v = part[pl.ds(PIECE * (i % TWO) + SUB * r, SUB), :]
        if extra is not None:
            v = v + extra[rows16(r), :].astype(F32)
        dst[rows16(r), :] = v.astype(BF16)


def rs_emit(p, s, part, sent, hop_l, hop_r, fin, own, ss, hl_rs, hr_rs, fin_rs):
    put = functools.partial(put_rows, part)
    for step in range(RS_STEPS):
        kind, pieces, blk = RS_PLAN[step][0], digits(RS_PLAN[step][ONE:]), RS_BLK[step]

        @pl.when(s == step)
        def _(kind=kind, pieces=pieces, blk=blk):
            for i in pieces:
                low, j = i < HALF_PC, i % HALF_PC
                if kind == 'X':
                    put(own.at[blk, half_of(i), :], i)
                    continue
                slot = 'ORL'.index(kind)
                dst = sent.at[slot, i]
                if kind == 'O':
                    put(dst, i)
                    hop, hop_rs, dev = (hop_l, hl_rs, p.right) if low else (hop_r, hr_rs, p.left)
                    rcopy(dst, hop.at[j], ss.at[slot, i], hop_rs.at[j], dev).start()
                    continue
                hop, hop_rs, dev, side = (hop_l, hl_rs, p.right, 0) if kind == 'R' else (hop_r, hr_rs, p.left, ONE)
                if low == (kind == 'R'):
                    rcopy(hop.at[j], hop.at[j], ss.at[slot, i], hop_rs.at[j], dev).wait_recv()
                    put(dst, i, hop.at[j])
                else:
                    put(dst, i)
                rcopy(dst, fin.at[side, i], ss.at[slot, i], fin_rs.at[side, i], dev).start()


def rs_wait_block(p, blk, sent, hop_l, hop_r, fin, own, ss, hl_rs, hr_rs, fin_rs):
    for side in range(TWO):
        for h in range(TWO):
            i = TWO * blk + h
            rcopy(fin.at[side, i], fin.at[side, i], ss.at[0, i], fin_rs.at[side, i], p.right).wait_recv()


def rs_total(blk, r, cols, fin, own):
    per = PIECE // SUB
    i, rows = TWO * blk + lax.div(r, per), rows16(lax.rem(r, per))
    total = (own[blk, rows16(r), cols].astype(F32) + fin[0, i, rows, cols].astype(F32)
             + fin[ONE, i, rows, cols].astype(F32))
    return total.astype(BF16).astype(F32)


def column_groups(width):
    return [pl.ds(QW * c, QW) for c in range(width // QW)]


def fold(val):
    out = val[:, :HD2]
    for c in range(ONE, QW // HD2):
        out = out + val[:, HD2 * c:HD2 * c + HD2]
    return out


def row_mean(parts, width):
    total = parts[0]
    for part in parts[ONE:]:
        total = total + part
    return jnp.sum(total, axis=1, keepdims=True) * (1.0 / width)


def rs_finish(p, sent, hop_l, hop_r, fin, own, ss, hl_rs, hr_rs, fin_rs):
    for slot in range(HALF_PC):
        for i in range(NPC):
            rcopy(sent.at[slot, i], sent.at[slot, i], ss.at[slot, i], fin_rs.at[0, i], p.right).wait_send()


def rope(lin, cos_t, sin_t):
    lo, hi = lin[:, :HD2], lin[:, HD2:]
    return jnp.concatenate([lo * cos_t - hi * sin_t, hi * cos_t + lo * sin_t], axis=1)


def rope_back(grad, cos_t, sin_t):
    lo, hi = grad[:, :HD2], grad[:, HD2:]
    return jnp.concatenate([lo * cos_t + hi * sin_t, hi * cos_t - lo * sin_t], axis=1)


def twice(row):
    return jnp.concatenate([row, row], axis=1)


def heads_down(row_pair):
    return jnp.concatenate([row_pair[:, :HD], row_pair[:, HD:]], axis=0)


def key_mask(pos_q, pos_k):
    gap = twice(pos_q) - twice(pos_k)
    return gap.astype(jnp.uint32) < jnp.uint32(WINDOW)


def head(n):
    return pl.ds(HD * n, HD)


def lanes_at(i, size):
    return pl.ds(pl.multiple_of(i * size, size), size)


def tiles_of(g):
    return lax.div(g * BLK, KT) + ONE


class Walk:
    def __init__(self, ga, gb):
        self.ga, self.gb = ga, gb
        self.na = tiles_of(ga)
        self.n = self.na + tiles_of(gb)
        self.turns = lax.div(self.n + ONE, TWO)

    def pos_q(self, i, pos_row):
        return jnp.where(i < self.n, pos_row, I32(-ONE))

    def at(self, i):
        i = jnp.minimum(jnp.maximum(i, 0), self.n - ONE)
        second = i >= self.na
        return (jnp.where(second, I32(ONE), I32(0)), jnp.where(second, self.gb, self.ga),
                jnp.where(second, i - self.na, i))


def store_columns(full, out, g, sem):
    for c in range(out.shape[0]):
        pltpu.make_async_copy(full.at[g, :, head(c)], out.at[c, g], sem).start()


class Loads:
    def __init__(self, sem):
        self.sem, self.count = sem, 0

    def add(self, src, dst):
        copy = pltpu.make_async_copy(src, dst, self.sem.at[self.count])
        copy.start()
        self.count += ONE
        return copy


def wait_all(copies):
    for copy in copies:
        copy.wait()


def gather_qkv_kernel(q_scale, x, pos_in, inv_freq, gain, wq, wk, wv, wo,
                      nall, q_out, k_out, v_out, kt_out, vt_out, cos_out, sin_out, posb_out, posr_out, wt_out, wtp_out,
                      wop_out, *scratch):
    n_ag = len(ag_scratch(BLK))
    ag, rest = scratch[:n_ag], scratch[n_ag:]
    (x_s, gain_s, wq_s, w_s, wt_s, q_s, k_s, v_s, kt_s, vt_s, cos_s, sin_s, posb_s, pos_s, lsem, osem, wsem, wo_sem, pos_ss,
     pos_rs, nall_sem) = rest
    full = ag[0]
    p = Place()
    loads = Loads(lsem)
    own = [loads.add(gain, gain_s.at[0])]
    own += [loads.add(x.at[i // TWO, half_of(i)], x_s.at[i // TWO, half_of(i)]) for i in AG_MADE]
    barrier(p.peers())

    def pos_copy(n, dev, owner):
        return rcopy(pos_in, pos_s.at[pl.ds(owner * NBLK, NBLK)], pos_ss.at[n], pos_rs.at[owner], dev)

    for n, dev in enumerate(p.peers()):
        pos_copy(n, dev, p.me).start()
    for b in range(NBLK):
        pos_s[p.me * NBLK + b] = pos_in[b]
    own[0].wait()
    for n, i in enumerate(AG_MADE):
        own[n + ONE].wait()
        if n == TWO:
            weights = [loads.add(wq, wq_s), loads.add(wk, w_s.at[:, pl.ds(QW, HD)]),
                       loads.add(wv, w_s.at[:, pl.ds(QW + HD, HD)])]
        b = i // TWO
        g = p.me * NBLK + b

        @pl.loop(0, PIECE // SUB)
        def _(r, b=b, g=g, start=PIECE * (i % TWO)):
            rows = pl.ds(start + SUB * r, SUB)
            val = x_s[b, rows, :].astype(F32)
            inv = lax.rsqrt(jnp.mean(val * val, axis=1, keepdims=True) + NORM_EPS)
            full[g, rows, :] = (val * inv * (1.0 + gain_s[...])).astype(BF16)

        for way, pieces in enumerate(AG_FIRST):
            if i in digits(pieces):
                ag_send(p, way, i, piece_of(full, p.me, i), *ag)
        if i in AG_MADE[TWO:CHIPS] + AG_MADE[-ONE:]:
            ag_swap(p, p.chip, b, full.at[g], full.at[g], *ag).start()
    wo_copy = rcopy(wo, wop_out, wo_sem.at[0], wo_sem.at[ONE], p.partner)
    wo_copy.start()
    for n, dev in enumerate(p.peers()):
        pos_copy(n, dev, dev).wait_recv()
    wait_all(weights)

    @pl.loop(0, w_s.shape[0] // BLK)
    def _(r):
        rows = lanes_at(r, BLK)
        both = wq_s[rows]
        for h in range(TWO):
            w_s[rows, head(h)] = both[:, h, :]

    def out_copies(g):
        tile, lanes = lax.div(g * BLK, KT), lanes_at(lax.rem(g, KT // BLK), BLK)
        return [(q_s.at[:, g], q_out.at[:, g]), (k_s.at[g], k_out.at[g]),
                (v_s.at[g], v_out.at[g]), (cos_s.at[g], cos_out.at[g]), (sin_s.at[g], sin_out.at[g]),
                (posb_s.at[g], posb_out.at[g]), (kt_s.at[tile, :, lanes], kt_out.at[tile, :, lanes]),
                (vt_s.at[tile, :, lanes], vt_out.at[tile, :, lanes])]

    whole = [(q_s, q_out), (k_s, k_out), (v_s, v_out), (cos_s, cos_out), (sin_s, sin_out),
             (posb_s, posb_out), (kt_s, kt_out), (vt_s, vt_out)]

    @pl.loop(0, AG_STEPS)
    def _(s):
        for n in range(TWO):
            g = ag_block(p, s, n)[-ONE]
            pos_row = pos_s[g]
            pos_b = jnp.broadcast_to(pos_row, (BLK, BLK)).T
            posr_out[g] = pos_row
            posb_s[g] = pos_b
            angle = pos_b.astype(F32) * inv_freq[...]
            cos_s[g] = jnp.cos(angle)
            sin_s[g] = jnp.sin(angle)
        pair = [ag_step(p, s, n, *ag) for n in range(TWO)]
        ag_then(s, lambda way, i: ag_send(p, way, i, piece_of(full, p.me, i), *ag))
        rows = jnp.concatenate([full[g] for g in pair], axis=0)
        for part in range(QKV // HD):
            lin = dot(rows, w_s[:, head(part)])
            for n, g in enumerate(pair):
                val = lin[BLK * n:BLK * n + BLK]
                tile, lanes = lax.div(g * BLK, KT), lanes_at(lax.rem(g, KT // BLK), BLK)
                if part < QW // HD:
                    q_s[part, g] = (rope(val, cos_s[g], sin_s[g]) * q_scale).astype(BF16)
                elif part == QW // HD:
                    val = rope(val, cos_s[g], sin_s[g])
                    k_s[g] = val.astype(BF16)
                    kt_s[tile, :, lanes] = val.T.astype(BF16)
                else:
                    v_s[g] = val.astype(BF16)
                    vt_s[tile, :, lanes] = val.T.astype(BF16)
        for g in pair:
            for n, (src, dst) in enumerate(out_copies(g)):
                pltpu.make_async_copy(src, dst, osem.at[n]).start()
            store_columns(full, nall, g, nall_sem)

        @pl.when(s == CHIPS)
        def _():
            @pl.loop(0, wt_s.shape[1] // HD)
            def _(j):
                wt_s[:, lanes_at(j, HD)] = w_s[lanes_at(j, HD), :].T

            pltpu.make_async_copy(wt_s, wt_out, wsem).start()
            rcopy(wt_s, wtp_out, wo_sem.at[TWO], wo_sem.at[TWO + ONE], p.partner).start()

    for n, (src, dst) in enumerate(whole):
        pltpu.make_async_copy(src, dst, osem.at[n]).wait()
    pltpu.make_async_copy(nall, nall, nall_sem).wait()
    pltpu.make_async_copy(wt_s, wt_out, wsem).wait()
    wo_copy.wait()
    rcopy(wt_s, wtp_out, wo_sem.at[TWO], wo_sem.at[TWO + ONE], p.partner).wait()
    for n, dev in enumerate(p.peers()):
        pos_copy(n, dev, dev).wait_send()
    ag_finish(p, *ag)


def attend_fwd_kernel(q, k, vt, posb, posr, wo, wop, x, gout, gain,
                      o_out, ot_out, lse_out, y_out, dproj_out, dgain_out, *scratch):
    n_rs = len(rs_scratch(BLK))
    rs, rest = scratch[:n_rs], scratch[n_rs:]
    (q_s, k_s, vt_s, posb_s, wo_s, gain_s, x_s, go_s, o_s, ot_s, op_s, part, qt, s_buf, e_buf, l_buf, acc, yst, dgain, row_a,
     row_b, lsem, op_ss, op_rs, osem, ysem) = rest
    fin, own = rs[HALF_PC], rs[HALF_PC + ONE]
    width = wo.shape[1]
    p = Place()
    loads = Loads(lsem)
    first = [loads.add(q, q_s), loads.add(k, k_s), loads.add(posb, posb_s), loads.add(vt, vt_s)]
    second = [loads.add(wo, wo_s.at[pl.ds(0, QW)]), loads.add(wop, wo_s.at[pl.ds(QW, QW)])]
    third = [loads.add(x, x_s), loads.add(gout, go_s), loads.add(gain, gain_s.at[0])]
    e_buf[...] = jnp.zeros_like(e_buf)
    barrier((p.right, p.left, p.partner))
    wait_all(first)

    def attend(pair, swap):
        walk = Walk(*pair)
        for n, g in enumerate(pair):
            qt[n] = q_s[:, g].reshape(TWO * BLK, HD).T
        acc[...] = jnp.zeros_like(acc)
        l_buf[...] = jnp.zeros_like(l_buf)

        def scores(i, a):
            n, _, t = walk.at(i)
            s_buf[a] = dot(k_s[t], qt[n])

        def values(i, a):
            n, _, t = walk.at(i)
            acc[n] += dot(vt_s[t], e_buf[a])

        def weights(i, a):
            n, g, t = walk.at(i)
            pos_q = walk.pos_q(i, posr[g])
            for c in range(KT // PIECE):
                keys = pl.ds(PIECE * c, PIECE)
                e = jnp.exp2(jnp.tanh(s_buf[a, keys, :] * (1.0 / SOFT_CAP)) * (SOFT_CAP * LOG2E))
                e = jnp.where(key_mask(pos_q, posb_s[t, keys, :]), e, 0.0)
                l_buf[n] += jnp.sum(e.reshape(PIECE // DEVS, DEVS, TWO * BLK), axis=0)
                e_buf[a, keys, :] = e.astype(BF16)

        def finish(n, g):
            l = jnp.sum(l_buf[n], axis=0, keepdims=True)
            lse_out[g] = jnp.log2(l)
            ot = acc[n] * (1.0 / l)
            for h in range(TWO):
                ot_s[h, :, lanes_at(g, BLK)] = ot[:, BLK * h:BLK * h + BLK].astype(BF16)
            o2 = ot.T.astype(BF16)
            for h in range(TWO):
                o_s[g, :, head(h)] = o2[BLK * h:BLK * h + BLK]

        scores(0, 0)

        @pl.loop(0, walk.turns)
        def _(turn):
            i = TWO * turn
            scores(i + ONE, ONE)
            values(i - ONE, ONE)
            weights(i, 0)
            scores(i + TWO, 0)
            values(i, 0)
            weights(i + ONE, ONE)

            @pl.when(lax.div(walk.na, TWO) == turn)
            def _():
                finish(0, walk.ga)
                swap.start()

        values(TWO * walk.turns - ONE, ONE)
        e_buf[...] = jnp.zeros_like(e_buf)
        finish(ONE, walk.gb)

    @pl.loop(0, RS_STEPS)
    def _(s):
        off, blk = pick(s, RS_OFF), pick(s, RS_BLK)
        chip = lax.rem(p.chip + off, CHIPS)
        mine = (TWO * chip + p.core) * NBLK + blk
        other = (TWO * chip + ONE - p.core) * NBLK + blk
        n = chip * NBLK + blk
        swap = rcopy(o_s.at[other], op_s.at[n], op_ss.at[n], op_rs.at[n], p.partner)
        attend((other, mine), swap)

        @pl.when(s == 0)
        def _():
            wait_all(second)

        swap.wait_recv()
        o_mine, o_part = o_s[mine], op_s[n]

        @pl.loop(0, TWO)
        def _(j):
            cols = lanes_at(j, width // TWO)
            part[:, cols] = dot(o_mine, wo_s[pl.ds(0, QW), cols]) + dot(o_part, wo_s[pl.ds(QW, QW), cols])

        rs_emit(p, s, part, *rs)

    outs = [pltpu.make_async_copy(o_s, o_out, osem.at[0]), pltpu.make_async_copy(ot_s, ot_out, osem.at[ONE])]
    for copy in outs:
        copy.start()
    wait_all(third)
    dgain[...] = jnp.zeros_like(dgain)
    for blk in RS_DONE:
        rs_wait_block(p, blk, *rs)

        @pl.loop(0, BLK // SUB)
        def _(r, blk=blk):
            rows, sums = rows16(r), []
            for cols in column_groups(width):
                val = rs_total(blk, r, cols, fin, own)
                row_a[:, cols] = val
                sums.append(fold(val * val))
            inv = lax.rsqrt(row_mean(sums, width) + NORM_EPS)
            sums = []
            for cols in column_groups(width):
                one_g = 1.0 + gain_s[:, cols]
                go = go_s[blk, rows, cols].astype(F32)
                nrm = row_a[:, cols] * inv
                post = (nrm * one_g).astype(BF16).astype(F32)
                yst[0, blk, rows, cols] = (x_s[blk, rows, cols].astype(F32) + post).astype(BF16)
                dg = go * nrm
                dgain[:, cols] += dg[:DEVS] + dg[DEVS:]
                gog = go * one_g
                row_a[:, cols] = nrm
                row_b[:, cols] = gog
                sums.append(fold(gog * nrm))
            mean = row_mean(sums, width)
            for cols in column_groups(width):
                yst[ONE, blk, rows, cols] = (inv * (row_b[:, cols] - row_a[:, cols] * mean)).astype(BF16)

        for n, dst in enumerate((y_out, dproj_out)):
            copy = pltpu.make_async_copy(yst.at[n, blk], dst.at[blk], ysem.at[n, blk])
            copy.start()
            outs.append(copy)
    dgain_out[...] = jnp.sum(dgain[...], axis=0, keepdims=True)
    for n in range(MY_BLK):
        rcopy(op_s.at[n], op_s.at[n], op_ss.at[n], op_rs.at[n], p.partner).wait_send()
    rs_finish(p, *rs)
    wait_all(outs)


def attend_bwd_kernel(q_scale, dproj, wo, q, k, kt, v, o, lse, cos_t, sin_t, posb, posr,
                      dall, dqkv_out, *scratch):
    n_ag = len(ag_scratch(BLK))
    ag, rest = scratch[:n_ag], scratch[n_ag:]
    (wo_s, q_s, k_s, kt_s, v_s, o_s, cos_s, sin_s, posb_s, dk_s, dv_s, dq_acc, out_s, qt, do_buf, dot_buf, delta, s_buf,
     dp_buf, p_buf, ds_buf, lsem, osem, own_sem) = rest
    full = ag[0]
    p = Place()
    loads = Loads(lsem)
    barrier((p.right, p.left, p.partner))

    def own_send(way, i):
        ag_send(p, way, i, dproj.at[i // TWO, half_of(i), :], *ag)

    for pieces in zip(*AG_FIRST):
        for way, i in enumerate(pieces):
            own_send(way, int(i))
    for b in range(NBLK):
        ag_swap(p, p.chip, b, dproj.at[b], full.at[p.me * NBLK + b], *ag).start()
    own = pltpu.make_async_copy(dproj, full.at[pl.ds(p.me * NBLK, NBLK)], own_sem)
    own.start()
    for src, dst in ((wo, wo_s), (o, o_s), (q, q_s), (k, k_s), (kt, kt_s), (v, v_s), (posb, posb_s), (cos_t, cos_s),
                     (sin_t, sin_s)):
        loads.add(src, dst)
    dk_s[...] = jnp.zeros_like(dk_s)
    dv_s[...] = jnp.zeros_like(dv_s)
    p_buf[...] = jnp.zeros_like(p_buf)
    ds_buf[...] = jnp.zeros_like(ds_buf)
    own.wait()
    for n, (src, dst) in enumerate(((wo, wo_s), (o, o_s), (q, q_s), (k, k_s), (kt, kt_s), (v, v_s), (posb, posb_s),
                                    (cos_t, cos_s), (sin_t, sin_s))):
        pltpu.make_async_copy(src, dst, lsem.at[n]).wait()
    dq_cols, kv_cols = pl.ds(0, QW), pl.ds(QW, QW)

    @pl.loop(0, AG_STEPS)
    def _(s):
        pair = [ag_step(p, s, n, *ag) for n in range(TWO)]
        ag_then(s, own_send)
        walk = Walk(*pair)
        for g in pair:
            store_columns(full, dall, g, osem.at[0])
        rows = jnp.concatenate([full[g] for g in pair], axis=0)
        do_all = dot_bt(rows, wo_s[...]).astype(BF16)
        for n, g in enumerate(pair):
            do2 = heads_down(do_all[BLK * n:BLK * n + BLK])
            do_buf[n] = do2
            dot_buf[n] = do2.T
            prod = do2.astype(F32) * heads_down(o_s[g]).astype(F32)
            delta[n] = jnp.sum(prod.T, axis=0, keepdims=True)
            qt[n] = q_s[:, g].reshape(TWO * BLK, HD).T
        dq_acc[...] = jnp.zeros_like(dq_acc)

        def scores(i, a):
            n, _, t = walk.at(i)
            s_buf[a] = dot(k_s[t], qt[n])
            dp_buf[a] = dot(v_s[t], dot_buf[n])

        def products(i, a):
            n, g, t = walk.at(i)
            dv_s[t] += dot(p_buf[a], do_buf[n])
            dk_s[t] += dot(ds_buf[a], q_s[:, g].reshape(TWO * BLK, HD))
            dq_acc[n] += dot(kt_s[t], ds_buf[a])

        def weights(i, a):
            n, g, t = walk.at(i)
            pos_q = walk.pos_q(i, posr[g])
            for c in range(KT // PIECE):
                keys = pl.ds(PIECE * c, PIECE)
                th = jnp.tanh(s_buf[a, keys, :] * (1.0 / SOFT_CAP))
                pr = jnp.exp2(th * (SOFT_CAP * LOG2E) - lse[g])
                pr = jnp.where(key_mask(pos_q, posb_s[t, keys, :]), pr, 0.0)
                p_buf[a, keys, :] = pr.astype(BF16)
                ds_buf[a, keys, :] = (pr * (dp_buf[a, keys, :] - delta[n]) * (1.0 - th * th)).astype(BF16)

        scores(0, 0)

        @pl.loop(0, walk.turns)
        def _(turn):
            i = TWO * turn
            scores(i + ONE, ONE)
            products(i - ONE, ONE)
            weights(i, 0)
            scores(i + TWO, 0)
            products(i, 0)
            weights(i + ONE, ONE)

        products(TWO * walk.turns - ONE, ONE)
        p_buf[...] = jnp.zeros_like(p_buf)
        ds_buf[...] = jnp.zeros_like(ds_buf)
        for n, g in enumerate(pair):
            dq = dq_acc[n].T
            for h in range(TWO):
                dq_h = rope_back(dq[BLK * h:BLK * h + BLK], cos_s[g], sin_s[g]) * q_scale
                out_s[g, :, head(h)] = dq_h.astype(BF16)
            pltpu.make_async_copy(out_s.at[g, :, dq_cols], dqkv_out.at[g, :, dq_cols], osem.at[ONE]).start()

    @pl.loop(0, ALL_BLK, unroll=CHIPS)
    def _(g):
        tile, rows = lax.div(g * BLK, KT), pl.ds(lax.rem(g, KT // BLK) * BLK, BLK)
        out_s[g, :, pl.ds(QW, HD)] = rope_back(dk_s[tile, rows, :], cos_s[g], sin_s[g]).astype(BF16)
        out_s[g, :, pl.ds(QW + HD, HD)] = dv_s[tile, rows, :].astype(BF16)
        pltpu.make_async_copy(out_s.at[g, :, kv_cols], dqkv_out.at[g, :, kv_cols], osem.at[TWO]).start()

    pltpu.make_async_copy(dall, dall, osem.at[0]).wait()
    pltpu.make_async_copy(out_s.at[:, :, dq_cols], dqkv_out.at[:, :, dq_cols], osem.at[ONE]).wait()
    pltpu.make_async_copy(out_s.at[:, :, kv_cols], dqkv_out.at[:, :, kv_cols], osem.at[TWO]).wait()
    ag_finish(p, *ag)


HOP_PLAN = ['O23', 'O01', 'O54', 'R54', 'L01', 'X01', 'X23', 'X45', 'R32', 'L23', 'R01', 'L54']
HOP_OFF, HOP_BLK = plan_tables(HOP_PLAN)
W_AHEAD = CHIPS
HOP_LATE = RS_STEPS - TWO
GROUPS = (digits('0145'), digits('23'))


def hop_emit(p, step, part, sent, turn, hop_l, hop_r, ss, hl_rs, hr_rs, result):
    kind = HOP_PLAN[step][0]
    for i in digits(HOP_PLAN[step][ONE:]):
        low, j = i < HALF_PC, i % HALF_PC
        hop, hop_rs, dev = (hop_l, hl_rs, p.right) if low else (hop_r, hr_rs, p.left)
        if kind == 'O':
            put_rows(part, sent.at[i], i)
            rcopy(sent.at[i], hop.at[j], ss.at[i], hop_rs.at[j], dev).start()
            continue
        n = 'RLX'.index(kind)
        if (kind == 'R' and low) or (kind == 'L' and not low):
            rcopy(hop.at[j], hop.at[j], ss.at[i], hop_rs.at[j], dev).wait_recv()
            put_rows(part, turn.at[n, i], i, hop.at[j])
        else:
            put_rows(part, turn.at[n, i], i)
        result(n, i).start()


def grad_rows_kernel(dqkv, wt, wtp, dg_post, *refs):
    n_out = TWO * len(GROUPS)
    hop_outs, (own_out, gpost_out), scratch = refs[:n_out], refs[n_out:n_out + TWO], refs[n_out + TWO:]
    (sent, turn, hop_l, hop_r, wt_s, d_s, dp_s, part, gains, ss, hl_rs, hr_rs, wt_sem, d_sem, dp_ss, dp_rs, out_sem, g_ss,
     g_rs, gsem) = scratch
    width = wt.shape[1]
    half, groups = width // TWO, width // QW
    p = Place()

    def w_loads(j):
        cols = lanes_at(j, QW)
        return [pltpu.make_async_copy(wt.at[:, cols], wt_s.at[pl.ds(0, QKV), cols], wt_sem.at[0, j]),
                pltpu.make_async_copy(wtp.at[:, cols], wt_s.at[pl.ds(QKV, QKV), cols], wt_sem.at[ONE, j])]

    def w_start(j):
        for copy in w_loads(j):
            copy.start()

    def block_of(off, blk, flip):
        chip = lax.rem(p.chip + off, CHIPS)
        return (TWO * chip + lax.rem(p.core + flip, TWO)) * NBLK + blk, chip * NBLK + blk

    def d_load(off, blk):
        g, n = block_of(off, blk, 0)
        return pltpu.make_async_copy(dqkv.at[g], d_s.at[n], d_sem.at[n])

    def d_swap(off, blk):
        other, n = block_of(off, blk, ONE)
        rcopy(dqkv.at[other], dp_s.at[n], dp_ss.at[n], dp_rs.at[n], p.partner).start()

    def result(n, i):
        dst = own_out.at[i]
        if n != TWO:
            group = [i in pieces for pieces in GROUPS].index(True)
            dst = hop_outs[n * len(GROUPS) + group].at[GROUPS[group].index(i)]
        return pltpu.make_async_copy(turn.at[n, i], dst, out_sem.at[n, i])

    plan = list(zip(HOP_OFF, HOP_BLK))
    d_load(*plan[0]).start()
    for j in range(W_AHEAD):
        w_start(j)
    barrier(p.peers())
    d_swap(*plan[0])
    send_gains(p, dg_post, gains, g_ss, g_rs)

    @pl.loop(0, RS_STEPS)
    def _(s):
        off, blk = pick(s, HOP_OFF), pick(s, HOP_BLK)
        _, n = block_of(off, blk, 0)
        late = jnp.where(s == HOP_LATE, I32(ONE), I32(0))
        d_load(off, blk).wait()
        rcopy(dp_s.at[n], dp_s.at[n], dp_ss.at[n], dp_rs.at[n], p.partner).wait_recv()
        d_mine, d_part = d_s[n], dp_s[n]

        def columns(cols):
            part[late, :, cols] = (dot(d_mine, wt_s[pl.ds(0, QKV), cols])
                                   + dot(d_part, wt_s[pl.ds(QKV, QKV), cols]))

        @pl.when(s == 0)
        def _():
            @pl.loop(0, groups)
            def _(j):
                @pl.when(j + W_AHEAD < groups)
                def _():
                    w_start(j + W_AHEAD)

                @pl.when(j + W_AHEAD == groups)
                def _():
                    for step in plan[ONE:]:
                        d_load(*step).start()
                        d_swap(*step)

                wait_all(w_loads(j))
                columns(lanes_at(j, QW))

        @pl.when(s != 0)
        def _():
            @pl.loop(0, TWO)
            def _(j):
                columns(lanes_at(j, half))

        @pl.when(s == RS_PLAN.index('X01'))
        def _():
            gain_total(p, dg_post, gains, gpost_out, g_ss, g_rs, gsem)

        for step in range(RS_STEPS):
            if step != HOP_LATE:
                @pl.when(s == step)
                def _(step=step):
                    if step > HOP_LATE:
                        hop_emit(p, HOP_LATE, part.at[ONE], sent, turn, hop_l, hop_r, ss, hl_rs, hr_rs, result)
                    hop_emit(p, step, part.at[0], sent, turn, hop_l, hop_r, ss, hl_rs, hr_rs, result)

    for i in range(NPC):
        rcopy(sent.at[i], sent.at[i], ss.at[i], hl_rs.at[0], p.right).wait_send()
    for n in range(MY_BLK):
        rcopy(dp_s.at[n], dp_s.at[n], dp_ss.at[n], dp_rs.at[n], p.partner).wait_send()
    for n in range(HALF_PC):
        for i in range(NPC):
            result(n, i).wait()


def gain_copy(n, src, gains, dev, owner, g_ss, g_rs):
    return rcopy(src, gains.at[owner], g_ss.at[n], g_rs.at[owner], dev)


def send_gains(p, src, gains, g_ss, g_rs):
    gains[p.me] = src[...]
    for n, dev in enumerate(p.peers()):
        gain_copy(n, src, gains, dev, p.me, g_ss, g_rs).start()


def gain_total(p, src, gains, out, g_ss, g_rs, gsem):
    for n, dev in enumerate(p.peers()):
        gain_copy(n, src, gains, dev, dev, g_ss, g_rs).wait()
    total = gains[0]
    for i in range(ONE, DEVS):
        total = total + gains[i]
    gains[p.me] = total
    copy = pltpu.make_async_copy(gains.at[p.me, 0], out, gsem)
    copy.start()
    copy.wait()


def weight_grads_kernel(dqkv, nall, dall, ot, y, gq_out, gk_out, gv_out, gwo_out, y_out, *scratch):
    d_s, in_s, gq_s, ot_s, gwo_s, y_s, lsem, isem, osem, wsem, ysem = scratch
    n_chunk = nall.shape[0]
    loads = Loads(lsem)
    first, second = loads.add(ot, ot_s), loads.add(y, y_s)
    d_copy = loads.add(dqkv, d_s)

    ahead = in_s.shape[0] - ONE

    def fetch(src, j, slot):
        pltpu.make_async_copy(src.at[j], in_s.at[slot], isem.at[slot]).start()

    def gwo_copies(j, slot):
        return [pltpu.make_async_copy(gwo_s.at[slot], gwo_out.at[:, lanes_at(j, HD)], wsem.at[slot])]

    def qkv_copies(j, slot):
        rows = lanes_at(j, HD)
        outs = (gq_out.at[rows, 0, :], gq_out.at[rows, ONE, :], gk_out.at[rows, 0, :], gv_out.at[rows, 0, :])
        return [pltpu.make_async_copy(gq_s.at[slot, :, head(n)], dst, osem.at[slot, n]) for n, dst in enumerate(outs)]

    def wo_chunk(a, slot):
        gwo_s[slot] = dot(ot_s[...], a)

    def qkv_chunk(a, slot):
        for h in range(TWO):
            cols = pl.ds(QW * h, QW)
            gq_s[slot, :, cols] = dot_at(a, d_s[:, :, cols].reshape(ALL_BLK * BLK, QW))

    def weight_grad(src, begun, after, compute, copies):
        @pl.loop(0, n_chunk)
        def _(j):
            at, slot = lax.rem(begun + j, ahead + ONE), lax.rem(j, TWO)
            pltpu.make_async_copy(src.at[j], in_s.at[at], isem.at[at]).wait()
            free = lax.rem(begun + j + ahead, ahead + ONE)

            @pl.when(j + ahead < n_chunk)
            def _():
                fetch(src, j + ahead, free)

            if after is not None:
                @pl.when(j + ahead >= n_chunk)
                def _():
                    fetch(after, j + ahead - n_chunk, free)

            @pl.when(j >= TWO)
            def _():
                wait_all(copies(j - TWO, slot))

            compute(in_s[at], slot)
            for copy in copies(j, slot):
                copy.start()

    for j in range(ahead):
        fetch(dall, j, j)
    first.wait()
    weight_grad(dall, 0, nall, wo_chunk, gwo_copies)
    d_copy.wait()
    second.wait()
    y_copy = pltpu.make_async_copy(y_s, y_out, ysem)
    y_copy.start()
    weight_grad(nall, n_chunk, None, qkv_chunk, qkv_copies)
    for j in (n_chunk - TWO, n_chunk - ONE):
        wait_all(gwo_copies(j, j % TWO) + qkv_copies(j, j % TWO))
    y_copy.wait()


def pre_load(pieces, from_left, from_right, own, x, gout, blocks, lsem):
    copies = []
    for m, i in enumerate(pieces):
        srcs = (from_left.at[m], from_right.at[m], own.at[i], x.at[i], gout.at[i])
        copies.append([pltpu.make_async_copy(src, blocks.at[n, m], lsem.at[n, m]) for n, src in enumerate(srcs)])
        for copy in copies[m]:
            copy.start()
    return copies


def pre_sums(blocks, m, gain, dn_s, stat, dgain):
    from_left, from_right, own, x, _ = (blocks.at[n, m] for n in range(blocks.shape[0]))
    width = x.shape[1]

    @pl.loop(0, PIECE // SUB)
    def _(r):
        rows, sums, dots = rows16(r), [], []
        for cols in column_groups(width):
            val = x[rows, cols].astype(F32)
            dn = (own[rows, cols].astype(F32) + from_left[rows, cols].astype(F32)
                  + from_right[rows, cols].astype(F32)).astype(BF16).astype(F32)
            dn_s[m, rows, cols] = dn
            sums.append(fold(val * val))
            dots.append(fold(dn * (1.0 + gain[:, cols]) * val))
        inv = lax.rsqrt(row_mean(sums, width) + NORM_EPS)
        stat[0, m, rows, :] = jnp.broadcast_to(inv, (SUB, HD2))
        stat[ONE, m, rows, :] = jnp.broadcast_to(row_mean(dots, width) * inv, (SUB, HD2))
        for cols in column_groups(width):
            dg = dn_s[m, rows, cols] * (x[rows, cols].astype(F32) * inv)
            dgain[:, cols] += dg[:DEVS] + dg[DEVS:]


def pre_result(blocks, m, gain, dn_s, stat, gx):
    x, gout = blocks.at[NBLK, m], blocks.at[NBLK + ONE, m]

    @pl.loop(0, PIECE // SUB)
    def _(r):
        rows = rows16(r)
        inv, mean = stat[0, m, rows, 0:1], stat[ONE, m, rows, 0:1]
        for cols in column_groups(x.shape[1]):
            nrm = x[rows, cols].astype(F32) * inv
            dx = (inv * (dn_s[m, rows, cols] * (1.0 + gain[:, cols]) - nrm * mean)).astype(BF16).astype(F32)
            gx[m, rows, cols] = (gout[rows, cols].astype(F32) + dx).astype(BF16)


def pre_grad_kernel(pieces, from_left, from_right, own, x, gout, gain, gx_out, dgain, blocks, gain_s, dn_s, stat, gx, lsem,
                    xsem, gsem):
    copies = pre_load(pieces, from_left, from_right, own, x, gout, blocks, lsem)
    gain_in = pltpu.make_async_copy(gain, gain_s.at[0], gsem)
    gain_in.start()
    dgain[...] = jnp.zeros_like(dgain)
    gain_in.wait()
    for m, i in enumerate(pieces):
        wait_all(copies[m])
        pre_sums(blocks, m, gain_s, dn_s, stat, dgain)
        pre_result(blocks, m, gain_s, dn_s, stat, gx)
        pltpu.make_async_copy(gx.at[m], gx_out.at[i], xsem.at[m]).start()
    for m, i in enumerate(pieces):
        pltpu.make_async_copy(gx.at[m], gx_out.at[i], xsem.at[m]).wait()


def pre_scratch(n, width):
    return [pltpu.VMEM((NBLK + TWO, n, PIECE, width), BF16), pltpu.VMEM((ONE, width), F32),
            pltpu.VMEM((n, PIECE, width), F32), pltpu.VMEM((TWO, n, PIECE, HD2), F32), pltpu.VMEM((n, PIECE, width), BF16),
            pltpu.SemaphoreType.DMA((NBLK + TWO, n))]


def pre_grad(pieces, *args):
    x, dma = args[NBLK], pltpu.SemaphoreType.DMA
    width = x.shape[TWO]
    return pl.pallas_call(
        functools.partial(pre_grad_kernel, pieces), name='pre_grad',
        out_shape=(sds(x.shape, BF16), sds((DEVS, width), F32)), in_specs=specs('AAAAAA'), out_specs=specs('AV'),
        scratch_shapes=pre_scratch(len(pieces), width) + [dma((len(pieces),)), dma(())],
        compiler_params=pltpu.CompilerParams(vmem_limit_bytes=VMEM_BYTES))(*args)


def last_rows_kernel(from_left, from_right, own, x, gout, gain, dgain_in, gx_out, gpre_out, *scratch):
    blocks, gain_s, dn_s, stat, gx, psem, dgain, row, gains, lsem, xsem, g_ss, g_rs, gsem = scratch
    pieces = GROUPS[ONE]
    p = Place()
    copies = pre_load(pieces, from_left, from_right, own, x, gout, blocks, psem)
    loads = Loads(lsem)
    rest = [loads.add(gain, gain_s.at[0]), loads.add(dgain_in, dgain)]
    barrier(p.peers())
    wait_all(rest)
    for m in range(len(pieces)):
        wait_all(copies[m])
        pre_sums(blocks, m, gain_s, dn_s, stat, dgain)
    row[...] = jnp.sum(dgain[...], axis=0, keepdims=True)
    send_gains(p, row, gains, g_ss, g_rs)
    for m in range(len(pieces)):
        pre_result(blocks, m, gain_s, dn_s, stat, gx)
    result = pltpu.make_async_copy(gx, gx_out, xsem)
    result.start()
    gain_total(p, row, gains, gpre_out, g_ss, g_rs, gsem)
    result.wait()


def finish_kernel(gx_last, gpre, gpost, gx_in, gx_out, gpre_out, gpost_out, blk_s, pre_s, post_s, get, put):
    moves = ((gx_last, blk_s, gx_out.at[pl.ds(GROUPS[ONE][0], len(GROUPS[ONE]))]), (gpre, pre_s, gpre_out), (gpost, post_s, gpost_out))
    for n, (src, buf, dst) in enumerate(moves):
        pltpu.make_async_copy(src, buf, get.at[n]).start()
    for n, (src, buf, dst) in enumerate(moves):
        pltpu.make_async_copy(src, buf, get.at[n]).wait()
        pltpu.make_async_copy(buf, dst, put.at[n]).start()
    for n, (src, buf, dst) in enumerate(moves):
        pltpu.make_async_copy(buf, dst, put.at[n]).wait()


def specs(places):
    return [pl.BlockSpec(memory_space={'A': pl.ANY, 'V': pltpu.VMEM}[place]) for place in places]


def params(cid):
    return pltpu.CompilerParams(collective_id=cid, has_side_effects=True, vmem_limit_bytes=VMEM_BYTES)


def sds(shape, dtype):
    return jax.ShapeDtypeStruct(shape, dtype)


def solution(mesh):
    act_spec = P('dp', 'tp', None)
    head_spec = P(None, 'tp', None)
    grad_spec = P('dp', 'tp', None)
    in_specs = (act_spec, P('dp', 'tp'), act_spec, head_spec, head_spec, head_spec, P('tp', None, None), P(None), P(None))
    out_specs = (act_spec, act_spec, grad_spec, grad_spec, grad_spec, P(('dp', 'tp'), None, None), P('dp'), P('dp'))
    assert mesh.shape['tp'] == DEVS

    def local_step(x_in, positions, grad_out, w_query, w_key, w_value, w_out, gain_pre, gain_post):
        width, _, head_dim = w_query.shape
        q_scale = head_dim ** -0.5
        rows = ALL_BLK * BLK
        tiles = rows // KT
        dma = pltpu.SemaphoreType.DMA
        vm = pltpu.VMEM
        x_blk = x_in.reshape(NBLK, BLK, width)
        go_blk = grad_out.reshape(NBLK, BLK, width)
        wo = w_out.reshape(QW, width)
        inv_freq = (ROPE_THETA ** (-2.0 * np.arange(HD2) / head_dim)).astype(np.float32).reshape(ONE, HD2)

        all_bf, rope_t = sds((width // HD, ALL_BLK, BLK, HD), BF16), sds((ALL_BLK, BLK, HD2), F32)
        blocks, tiles_t = sds((ALL_BLK, BLK, HD), BF16), sds((tiles, HD, KT), BF16)
        pos_blk, pos_row = sds((ALL_BLK, BLK, HD2), I32), sds((ALL_BLK, ONE, HD2), I32)
        q_all, w_t, own_rows = sds((TWO, ALL_BLK, BLK, HD), BF16), sds((QKV, width), BF16), sds(x_blk.shape, BF16)
        o_all, ot_all, lse_all = sds((ALL_BLK, BLK, QW), BF16), sds((TWO, HD, rows), BF16), sds((ALL_BLK, ONE, HD), F32)
        d_all, gain_row = sds((ALL_BLK, BLK, QKV), BF16), sds((ONE, width), F32)

        def like(*specs):
            return [vm(spec.shape, spec.dtype) for spec in specs]

        (nall, q, k, v, kt, vt, cos_t, sin_t, posb, posr, wt, wtp, wop) = pl.pallas_call(
            functools.partial(gather_qkv_kernel, q_scale), name='gather_qkv',
            out_shape=(all_bf, q_all, blocks, blocks, tiles_t, tiles_t, rope_t, rope_t, pos_blk, pos_row, w_t, w_t,
                       sds(wo.shape, BF16)),
            in_specs=specs('AVVAAAAA'), out_specs=specs('AAAAAAAAAVAAA'),
            scratch_shapes=ag_scratch(width) + like(
                own_rows, gain_row, sds(w_query.shape, BF16), sds((width, QKV), BF16), w_t, q_all, blocks, blocks, tiles_t, tiles_t, rope_t, rope_t,
                pos_blk, pos_row) + [dma((10,)), dma((9,)), dma(()), dma((CHIPS,)), dma((DEVS,)), dma((DEVS,)), dma(())],
            compiler_params=params(0),
        )(x_blk, positions.reshape(NBLK, ONE, BLK), inv_freq, gain_pre, w_query, w_key.reshape(width, HD), w_value.reshape(width, HD), wo)

        k_t, v_t, posb_t = (a.reshape(tiles, KT, a.shape[2]) for a in (k, v, posb))
        tile_rows, tile_f = sds(k_t.shape, BF16), sds(k_t.shape, F32)
        tile_pos, score, square = sds(posb_t.shape, I32), sds((TWO, KT, HD), F32), sds((TWO, HD, HD), BF16)
        square_f, part = sds((TWO, HD, HD), F32), sds((BLK, width), F32)
        o, ot, lse, y, dproj, dg_post = pl.pallas_call(
            attend_fwd_kernel, name='attend_fwd',
            out_shape=(o_all, ot_all, lse_all, own_rows, own_rows, gain_row),
            in_specs=specs('AAAAVAAAAA'), out_specs=specs('AAVAAV'),
            scratch_shapes=rs_scratch(width) + like(
                q_all, tile_rows, tiles_t, tile_pos, w_t, gain_row, own_rows, own_rows, o_all, ot_all,
                sds((MY_BLK, BLK, QW), BF16), part, square, score, sds(score.shape, BF16), sds((TWO, DEVS, HD), F32),
                square_f, sds((TWO,) + x_blk.shape, BF16), sds((DEVS, width), F32), sds((SUB, width), F32),
                sds((SUB, width), F32))
            + [dma((9,)), dma((MY_BLK,)), dma((MY_BLK,)), dma((TWO,)), dma((TWO, NBLK))],
            compiler_params=params(1),
        )(q, k_t, vt, posb_t, posr, wo, wop, x_blk, go_blk, gain_post)

        dall, dqkv = pl.pallas_call(
            functools.partial(attend_bwd_kernel, q_scale), name='attend_bwd',
            out_shape=(all_bf, d_all),
            in_specs=specs('AAAAAAAVAAAV'), out_specs=specs('AA'),
            scratch_shapes=ag_scratch(width) + like(
                sds(wo.shape, BF16), q_all, tile_rows, tiles_t, tile_rows, o_all, rope_t, rope_t, tile_pos, tile_f, tile_f,
                square_f, d_all, square, square, square, sds((TWO, ONE, HD), F32), score, score, sds(score.shape, BF16),
                sds(score.shape, BF16)) + [dma((9,)), dma((3,)), dma(())],
            compiler_params=params(2),
        )(dproj, wo, q, k_t, kt, v_t, o, lse, cos_t, sin_t, posb_t, posr)

        hops = [sds((len(pieces), PIECE, width), BF16) for pieces in GROUPS]
        piece, own_pieces = sds((HALF_PC, PIECE, width), BF16), sds((NPC, PIECE, width), BF16)
        gain_all, d_mine = sds((DEVS, ONE, width), F32), sds((MY_BLK, BLK, QKV), BF16)
        *to_all, own, gpost = pl.pallas_call(
            grad_rows_kernel, name='grad_rows',
            out_shape=hops + hops + [own_pieces, sds((width,), F32)],
            in_specs=specs('AAAV'), out_specs=specs('AAAAAA'),
            scratch_shapes=like(
                own_pieces, sds((HALF_PC, NPC, PIECE, width), BF16), piece, piece,
                sds((TWO * QKV, width), BF16), d_mine, d_mine, sds((TWO, BLK, width), F32), gain_all)
            + [dma((NPC,)), dma((HALF_PC,)), dma((HALF_PC,)), dma((TWO, width // QW)), dma((MY_BLK,)),
               dma((MY_BLK,)), dma((MY_BLK,)), dma((HALF_PC, NPC)), dma((DEVS,)), dma((DEVS,)), dma(())],
            compiler_params=params(3),
        )(dqkv, wt, wtp, dg_post)

        def shift(rows_out, way):
            ring = [(TWO * c + k, TWO * ((c + way) % CHIPS) + k) for c in range(CHIPS) for k in range(TWO)]
            return lax.ppermute(rows_out, 'tp', ring)

        hops_in = []
        for n in range(len(GROUPS)):
            hops_in.append((shift(to_all[n], ONE), shift(to_all[n + len(GROUPS)], CHIPS - ONE)))
        flops = TWO * rows * width * (QKV + QW)
        gq, gk, gv, gwo, y = pl.pallas_call(
            weight_grads_kernel, name='weight_grads',
            out_shape=(sds(w_query.shape, F32), sds(w_key.shape, F32), sds(w_value.shape, F32), sds(wo.shape, F32),
                       own_rows),
            in_specs=specs('AAAAA'), out_specs=specs('AAAAA'),
            scratch_shapes=like(
                d_all, sds((CHIPS, rows, HD), BF16), sds((TWO, HD, QKV), F32), sds((QW, rows), BF16), sds((TWO, QW, HD), F32),
                own_rows) + [dma((3,)), dma((CHIPS,)), dma((TWO, CHIPS)), dma((TWO,)), dma(())],
            cost_estimate=pl.CostEstimate(flops=flops, bytes_accessed=TWO * rows * width * CHIPS, transcendentals=0),
            compiler_params=pltpu.CompilerParams(vmem_limit_bytes=VMEM_BYTES),
        )(dqkv, *(a.reshape(width // HD, rows, HD) for a in (nall, dall)), ot.reshape(QW, rows), y)
        x_pc, go_pc = x_in.reshape(NPC, PIECE, width), grad_out.reshape(NPC, PIECE, width)
        gx, dgain = pre_grad(GROUPS[0], *hops_in[0], own, x_pc, go_pc, gain_pre)
        block = hops[ONE]
        gx_last, gpre = pl.pallas_call(
            last_rows_kernel, name='last_rows', out_shape=(block, sds((width,), F32)),
            in_specs=specs('AAAAAAA'), out_specs=specs('AA'),
            scratch_shapes=pre_scratch(block.shape[0], width) + like(sds((DEVS, width), F32), gain_row, gain_all)
            + [dma((TWO,)), dma(()), dma((DEVS,)), dma((DEVS,)), dma(())],
            compiler_params=params(4),
        )(*hops_in[ONE], own, x_pc, go_pc, gain_pre, dgain)
        gx, gpre, gpost = pl.pallas_call(
            finish_kernel, name='finish', out_shape=(own_pieces, sds((width,), F32), sds((width,), F32)),
            in_specs=specs('AAAA'), out_specs=specs('AAA'), input_output_aliases={3: 0},
            scratch_shapes=like(block, sds((width,), F32), sds((width,), F32)) + [dma((3,)), dma((3,))],
            compiler_params=pltpu.CompilerParams(vmem_limit_bytes=VMEM_BYTES),
        )(gx_last, gpre, gpost, gx)
        return (y.reshape(x_in.shape), gx.reshape(x_in.shape), gq, gk, gv, gwo.reshape(w_out.shape), gpre, gpost)

    return jax.shard_map(local_step, mesh=mesh, in_specs=in_specs, out_specs=out_specs, check_vma=False)
```

```python
import functools

import jax
import jax.numpy as jnp
import numpy as np
from jax import lax
from jax.experimental import pallas as pl
from jax.experimental.pallas import tpu as pltpu
from jax.sharding import PartitionSpec as P


WINDOW = 4096
SOFT_CAP = 50.0
NORM_EPS = 1e-6
ROPE_THETA = 10000.0
LOG2E = 1.4426950408889634
BLK = 128
PIECE = 64
SUB = 16
KT = 512
NBLK = 3
NPC = 6
HALF_PC = 3
CHIPS = 4
DEVS = 8
ALL_BLK = DEVS * NBLK
MY_BLK = CHIPS * NBLK
HD = 256
HD2 = 128
QW = 512
QKV = 1024
ONE, TWO = 1, 2
VMEM_BYTES = 67 * 1000 * 1000
F32 = jnp.float32
BF16 = jnp.bfloat16
I32 = jnp.int32


def dot(a, b):
    return lax.dot_general(a, b, (((1,), (0,)), ((), ())), preferred_element_type=F32)


def dot_bt(a, b):
    return lax.dot_general(a, b, (((1,), (1,)), ((), ())), preferred_element_type=F32)


def dot_at(a, b):
    return lax.dot_general(a, b, (((0,), (0,)), ((), ())), preferred_element_type=F32)


def pick(s, values):
    out = I32(values[0])
    for i, value in enumerate(values):
        if value != values[0]:
            out = jnp.where(s == i, I32(value), out)
    return out


def rcopy(src, dst, ss, rs, dev):
    return pltpu.make_async_remote_copy(src_ref=src, dst_ref=dst, send_sem=ss, recv_sem=rs,
                                        device_id={'tp': dev}, device_id_type=pl.DeviceIdType.MESH)


class Place:
    def __init__(self):
        me = lax.axis_index('tp')
        self.me = me
        self.chip = lax.div(me, TWO)
        self.core = lax.rem(me, TWO)
        self.right = self.dev(ONE, 0)
        self.left = self.dev(CHIPS - ONE, 0)
        self.partner = self.dev(0, ONE)

    def dev(self, chip_off, flip):
        chip = lax.rem(self.chip + chip_off, CHIPS)
        return TWO * chip + lax.rem(self.core + flip, TWO)

    def peers(self):
        return [lax.rem(self.me + d, DEVS) for d in range(ONE, DEVS)]


def barrier(devs):
    sem = pltpu.get_barrier_semaphore()
    for dev in devs:
        pl.semaphore_signal(sem, inc=ONE, device_id={'tp': dev}, device_id_type=pl.DeviceIdType.MESH)
    pl.semaphore_wait(sem, len(devs))


def rows16(r):
    return pl.ds(SUB * r, SUB)


def digits(text):
    return [int(c) for c in text]


AG_OFF = (digits('003033322332'), digits('001011122112'))
AG_FLIP = (digits('000110101010'), digits('010110101011'))
AG_BLK = (digits('020101100221'), digits('102221122001'))
AG_STEPS = len(AG_OFF[0])
AG_LAST = AG_STEPS - ONE
AG_FORWARD = {2: ('01', '54'), 5: ('2', '3')}
AG_FIRST = ('0123', '5432')
AG_THEN = ('45', '10')
AG_MADE = digits('051432')
AG_THEN_STEP = 2


def ag_scratch(width):
    dma = pltpu.SemaphoreType.DMA
    return [pltpu.VMEM((ALL_BLK, BLK, width), BF16),
            dma((CHIPS, NPC)),
            dma((CHIPS, NBLK)),
            dma((TWO, NPC)),
            dma((NPC,)),
            dma((CHIPS, NBLK))]


def half_of(i):
    return pl.ds(PIECE * (i % TWO), PIECE)


def piece_of(full, shard, i):
    return full.at[shard * NBLK + i // TWO, half_of(i), :]


def ag_send(p, way, i, src, full, ring_rs, part_rs, own_ss, fwd_ss, part_ss):
    rcopy(src, piece_of(full, p.me, i), own_ss.at[way, i], ring_rs.at[p.chip, i], (p.right, p.left)[way]).start()


def ag_then(s, src):
    @pl.when(s == AG_THEN_STEP)
    def _():
        for way, pieces in enumerate(AG_THEN):
            for i in digits(pieces):
                src(way, i)


def ag_swap(p, chip, blk, src, dst, full, ring_rs, part_rs, own_ss, fwd_ss, part_ss):
    return rcopy(src, dst, part_ss.at[chip, blk], part_rs.at[chip, blk], p.partner)


def ag_block(p, s, n):
    off, flip, blk = pick(s, AG_OFF[n]), pick(s, AG_FLIP[n]), pick(s, AG_BLK[n])
    chip = lax.rem(p.chip + off, CHIPS)
    shard = TWO * chip + lax.rem(p.core + flip, TWO)
    return off, flip, chip, shard, blk, shard * NBLK + blk


def ag_arrive(p, chip, blk, g, full, ring_rs, part_rs, own_ss, fwd_ss, part_ss):
    for h in range(TWO):
        half = full.at[g, half_of(h), :]
        rcopy(half, half, fwd_ss.at[0], ring_rs.at[chip, TWO * blk + h], p.partner).wait_recv()
    rcopy(full.at[g], full.at[g], part_ss.at[chip, blk], part_rs.at[chip, blk], p.partner).start()


def ag_last(p, *ag):
    _, _, chip, _, blk, g = ag_block(p, AG_LAST, 0)
    ag_arrive(p, chip, blk, g, *ag)


def ag_step(p, s, n, full, ring_rs, part_rs, own_ss, fwd_ss, part_ss):
    off, flip, chip, shard, blk, g = ag_block(p, s, n)
    swap = rcopy(full.at[g], full.at[g], part_ss.at[chip, blk], part_rs.at[chip, blk], p.partner)

    @pl.when(flip != 0)
    def _():
        swap.wait_recv()

    ring = jnp.logical_and(flip == 0, off != 0)

    @pl.when(ring if n else jnp.logical_and(ring, s != AG_LAST))
    def _():
        ag_arrive(p, chip, blk, g, full, ring_rs, part_rs, own_ss, fwd_ss, part_ss)

    for step, pieces in AG_FORWARD.items():
        @pl.when(s == step)
        def _(pieces=pieces[n]):
            for i in digits(pieces):
                ref = piece_of(full, shard, i)
                rcopy(ref, ref, fwd_ss.at[i], ring_rs.at[chip, i], (p.right, p.left)[n]).start()
    return g


def ag_finish(p, full, ring_rs, part_rs, own_ss, fwd_ss, part_ss):
    for n in range(NPC):
        ref = piece_of(full, p.me, n)
        for sem in (own_ss.at[0, n], own_ss.at[ONE, n], fwd_ss.at[n]):
            rcopy(ref, ref, sem, ring_rs.at[p.chip, n], p.right).wait_send()
    for c in range(CHIPS):
        for b in range(NBLK):
            ref = full.at[b]
            rcopy(ref, ref, part_ss.at[c, b], part_rs.at[c, b], p.partner).wait_send()


RS_PLAN = ['O23', 'O01', 'O54', 'R54', 'L01', 'X01', 'X23', 'X45', 'R01', 'L54', 'R32', 'L23']


def plan_tables(plan):
    return ([{'O': TWO, 'R': ONE, 'L': CHIPS - ONE, 'X': 0}[step[0]] for step in plan],
            [int(step[ONE]) // TWO for step in plan])


RS_OFF, RS_BLK = plan_tables(RS_PLAN)
RS_STEPS = len(RS_PLAN)
RS_DONE = digits('021')


def rs_scratch(width):
    dma = pltpu.SemaphoreType.DMA
    return [pltpu.VMEM((HALF_PC, NPC, PIECE, width), BF16),
            pltpu.VMEM((HALF_PC, PIECE, width), BF16),
            pltpu.VMEM((HALF_PC, PIECE, width), BF16),
            pltpu.VMEM((TWO, NPC, PIECE, width), BF16),
            pltpu.VMEM((NBLK, BLK, width), BF16),
            dma((HALF_PC, NPC)), dma((HALF_PC,)), dma((HALF_PC,)), dma((TWO, NPC))]


def put_rows(part, dst, i, extra=None):
    @pl.loop(0, PIECE // SUB)
    def _(r):
        v = part[pl.ds(PIECE * (i % TWO) + SUB * r, SUB), :]
        if extra is not None:
            v = v + extra[rows16(r), :].astype(F32)
        dst[rows16(r), :] = v.astype(BF16)


def rs_emit(p, s, part, sent, hop_l, hop_r, fin, own, ss, hl_rs, hr_rs, fin_rs):
    put = functools.partial(put_rows, part)
    for step in range(RS_STEPS):
        kind, pieces, blk = RS_PLAN[step][0], digits(RS_PLAN[step][ONE:]), RS_BLK[step]

        @pl.when(s == step)
        def _(kind=kind, pieces=pieces, blk=blk):
            for i in pieces:
                low, j = i < HALF_PC, i % HALF_PC
                if kind == 'X':
                    put(own.at[blk, half_of(i), :], i)
                    continue
                slot = 'ORL'.index(kind)
                dst = sent.at[slot, i]
                if kind == 'O':
                    put(dst, i)
                    hop, hop_rs, dev = (hop_l, hl_rs, p.right) if low else (hop_r, hr_rs, p.left)
                    rcopy(dst, hop.at[j], ss.at[slot, i], hop_rs.at[j], dev).start()
                    continue
                hop, hop_rs, dev, side = (hop_l, hl_rs, p.right, 0) if kind == 'R' else (hop_r, hr_rs, p.left, ONE)
                if low == (kind == 'R'):
                    rcopy(hop.at[j], hop.at[j], ss.at[slot, i], hop_rs.at[j], dev).wait_recv()
                    put(dst, i, hop.at[j])
                else:
                    put(dst, i)
                rcopy(dst, fin.at[side, i], ss.at[slot, i], fin_rs.at[side, i], dev).start()


def rs_wait_block(p, blk, sent, hop_l, hop_r, fin, own, ss, hl_rs, hr_rs, fin_rs):
    for side in range(TWO):
        for h in range(TWO):
            i = TWO * blk + h
            rcopy(fin.at[side, i], fin.at[side, i], ss.at[0, i], fin_rs.at[side, i], p.right).wait_recv()


def rs_total(blk, fin, own, r, cols):
    per = PIECE // SUB
    i, rows = TWO * blk + lax.div(r, per), rows16(lax.rem(r, per))
    total = (own[blk, rows16(r), cols].astype(F32) + fin[0, i, rows, cols].astype(F32)
             + fin[ONE, i, rows, cols].astype(F32))
    return total.astype(BF16).astype(F32)


def column_groups(width):
    return [pl.ds(QW * c, QW) for c in range(width // QW)]


def fold(val):
    out = val[:, :HD2]
    for c in range(ONE, QW // HD2):
        out = out + val[:, HD2 * c:HD2 * c + HD2]
    return out


def row_mean(parts, width):
    total = parts[0]
    for part in parts[ONE:]:
        total = total + part
    return jnp.sum(total, axis=1, keepdims=True) * (1.0 / width)


def post_rows(total, x, gout, gain, y, dproj, dgain, row_a, row_b):
    width = x.shape[1]

    @pl.loop(0, BLK // SUB)
    def _(r):
        rows, sums = rows16(r), []
        for cols in column_groups(width):
            val = total(r, cols)
            row_a[:, cols] = val
            sums.append(fold(val * val))
        inv = lax.rsqrt(row_mean(sums, width) + NORM_EPS)
        sums = []
        for cols in column_groups(width):
            one_g = 1.0 + gain[:, cols]
            go = gout[rows, cols].astype(F32)
            nrm = row_a[:, cols] * inv
            post = (nrm * one_g).astype(BF16).astype(F32)
            y[rows, cols] = (x[rows, cols].astype(F32) + post).astype(BF16)
            dg = go * nrm
            dgain[:, cols] += dg[:DEVS] + dg[DEVS:]
            gog = go * one_g
            row_a[:, cols] = nrm
            row_b[:, cols] = gog
            sums.append(fold(gog * nrm))
        mean = row_mean(sums, width)
        for cols in column_groups(width):
            dproj[rows, cols] = (inv * (row_b[:, cols] - row_a[:, cols] * mean)).astype(BF16)


def rs_finish(p, sent, hop_l, hop_r, fin, own, ss, hl_rs, hr_rs, fin_rs):
    for slot in range(HALF_PC):
        for i in range(NPC):
            rcopy(sent.at[slot, i], sent.at[slot, i], ss.at[slot, i], fin_rs.at[0, i], p.right).wait_send()


def rope(lin, cos_t, sin_t):
    lo, hi = lin[:, :HD2], lin[:, HD2:]
    return jnp.concatenate([lo * cos_t - hi * sin_t, hi * cos_t + lo * sin_t], axis=1)


def rope_back(grad, cos_t, sin_t):
    lo, hi = grad[:, :HD2], grad[:, HD2:]
    return jnp.concatenate([lo * cos_t + hi * sin_t, hi * cos_t - lo * sin_t], axis=1)


def twice(row):
    return jnp.concatenate([row, row], axis=1)


def heads_down(row_pair):
    return jnp.concatenate([row_pair[:, :HD], row_pair[:, HD:]], axis=0)


def key_mask(pos_q, pos_k):
    gap = twice(pos_q) - twice(pos_k)
    return gap.astype(jnp.uint32) < jnp.uint32(WINDOW)


def head(n):
    return pl.ds(HD * n, HD)


def lanes_at(i, size):
    return pl.ds(pl.multiple_of(i * size, size), size)


def tiles_of(g):
    return lax.div(g * BLK, KT) + ONE


class Walk:
    def __init__(self, ga, gb):
        self.ga, self.gb = ga, gb
        self.na = tiles_of(ga)
        self.n = self.na + tiles_of(gb)
        self.turns = lax.div(self.n + ONE, TWO)

    def pos_q(self, i, pos_row):
        return jnp.where(i < self.n, pos_row, I32(-ONE))

    def at(self, i):
        i = jnp.minimum(jnp.maximum(i, 0), self.n - ONE)
        second = i >= self.na
        return (jnp.where(second, I32(ONE), I32(0)), jnp.where(second, self.gb, self.ga),
                jnp.where(second, i - self.na, i))


def store_columns(full, out, g, sem):
    for c in range(out.shape[0]):
        pltpu.make_async_copy(full.at[g, :, head(c)], out.at[c, g], sem).start()


class Loads:
    def __init__(self, sem):
        self.sem, self.count = sem, 0

    def add(self, src, dst):
        copy = pltpu.make_async_copy(src, dst, self.sem.at[self.count])
        copy.start()
        self.count += ONE
        return copy


def wait_all(copies):
    for copy in copies:
        copy.wait()


def gather_qkv_kernel(q_scale, x, pos_in, inv_freq, gain, wq, wk, wv, wo,
                      nall, q_out, k_out, v_out, kt_out, vt_out, cos_out, sin_out, posb_out, posr_out, wt_out, wtp_out,
                      wop_out, *scratch):
    n_ag = len(ag_scratch(BLK))
    ag, rest = scratch[:n_ag], scratch[n_ag:]
    (x_s, gain_s, wq_s, w_s, wt_s, q_s, k_s, v_s, kt_s, vt_s, cos_s, sin_s, posb_s, pos_s, lsem, osem, wsem, wo_sem, pos_ss,
     pos_rs, nall_sem) = rest
    full = ag[0]
    p = Place()
    loads = Loads(lsem)
    own = [loads.add(gain, gain_s.at[0])]
    own += [loads.add(x.at[i // TWO, half_of(i)], x_s.at[i // TWO, half_of(i)]) for i in AG_MADE]
    barrier(p.peers())

    def pos_copy(n, dev, owner):
        return rcopy(pos_in, pos_s.at[pl.ds(owner * NBLK, NBLK)], pos_ss.at[n], pos_rs.at[owner], dev)

    for n, dev in enumerate(p.peers()):
        pos_copy(n, dev, p.me).start()
    for b in range(NBLK):
        pos_s[p.me * NBLK + b] = pos_in[b]
    own[0].wait()
    for n, i in enumerate(AG_MADE):
        own[n + ONE].wait()
        if n == TWO:
            weights = [loads.add(wq, wq_s), loads.add(wk, w_s.at[:, pl.ds(QW, HD)]),
                       loads.add(wv, w_s.at[:, pl.ds(QW + HD, HD)])]
        b = i // TWO
        g = p.me * NBLK + b

        @pl.loop(0, PIECE // SUB)
        def _(r, b=b, g=g, start=PIECE * (i % TWO)):
            rows = pl.ds(start + SUB * r, SUB)
            val = x_s[b, rows, :].astype(F32)
            inv = lax.rsqrt(jnp.mean(val * val, axis=1, keepdims=True) + NORM_EPS)
            full[g, rows, :] = (val * inv * (1.0 + gain_s[...])).astype(BF16)

        for way, pieces in enumerate(AG_FIRST):
            if i in digits(pieces):
                ag_send(p, way, i, piece_of(full, p.me, i), *ag)
        if i in AG_MADE[TWO:CHIPS] + AG_MADE[-ONE:]:
            ag_swap(p, p.chip, b, full.at[g], full.at[g], *ag).start()
    wo_copy = rcopy(wo, wop_out, wo_sem.at[0], wo_sem.at[ONE], p.partner)
    wo_copy.start()
    for n, dev in enumerate(p.peers()):
        pos_copy(n, dev, dev).wait_recv()
    wait_all(weights)

    @pl.loop(0, w_s.shape[0] // BLK)
    def _(r):
        rows = lanes_at(r, BLK)
        both = wq_s[rows]
        for h in range(TWO):
            w_s[rows, head(h)] = both[:, h, :]

    def out_copies(g):
        tile, lanes = lax.div(g * BLK, KT), lanes_at(lax.rem(g, KT // BLK), BLK)
        return [(cos_s.at[g], cos_out.at[g]), (sin_s.at[g], sin_out.at[g]), (posb_s.at[g], posb_out.at[g]),
                (q_s.at[:, g], q_out.at[:, g]), (k_s.at[g], k_out.at[g]), (v_s.at[g], v_out.at[g]),
                (kt_s.at[tile, :, lanes], kt_out.at[tile, :, lanes]), (vt_s.at[tile, :, lanes], vt_out.at[tile, :, lanes])]

    whole = [(cos_s, cos_out), (sin_s, sin_out), (posb_s, posb_out), (q_s, q_out), (k_s, k_out), (v_s, v_out),
             (kt_s, kt_out), (vt_s, vt_out)]
    n_rope = NBLK

    def store(g, late):
        for n, (src, dst) in enumerate(out_copies(g)):
            if late == (n >= n_rope):
                pltpu.make_async_copy(src, dst, osem.at[n]).start()

    def products(blocks):
        for g in blocks:
            store_columns(full, nall, g, nall_sem)
        rows = jnp.concatenate([full[g] for g in blocks], axis=0) if len(blocks) > ONE else full[blocks[0]]
        for part in range(QKV // HD):
            lin = dot(rows, w_s[:, head(part)])
            for n, g in enumerate(blocks):
                val = lin[BLK * n:BLK * n + BLK]
                tile, lanes = lax.div(g * BLK, KT), lanes_at(lax.rem(g, KT // BLK), BLK)
                if part < QW // HD:
                    q_s[part, g] = (rope(val, cos_s[g], sin_s[g]) * q_scale).astype(BF16)
                elif part == QW // HD:
                    val = rope(val, cos_s[g], sin_s[g])
                    k_s[g] = val.astype(BF16)
                    kt_s[tile, :, lanes] = val.T.astype(BF16)
                else:
                    v_s[g] = val.astype(BF16)
                    vt_s[tile, :, lanes] = val.T.astype(BF16)
        for g in blocks:
            store(g, True)

    @pl.loop(0, AG_STEPS)
    def _(s):
        for n in range(TWO):
            g = ag_block(p, s, n)[-ONE]
            pos_row = pos_s[g]
            pos_b = jnp.broadcast_to(pos_row, (BLK, BLK)).T
            posr_out[g] = pos_row
            posb_s[g] = pos_b
            angle = pos_b.astype(F32) * inv_freq[...]
            cos_s[g] = jnp.cos(angle)
            sin_s[g] = jnp.sin(angle)
            store(g, False)

        @pl.when(s == AG_LAST)
        def _():
            ag_last(p, *ag)
            products([ag_block(p, s, 0)[-ONE]])
            products([ag_step(p, s, ONE, *ag)])

        @pl.when(s != AG_LAST)
        def _():
            pair = [ag_step(p, s, n, *ag) for n in range(TWO)]
            ag_then(s, lambda way, i: ag_send(p, way, i, piece_of(full, p.me, i), *ag))
            products(pair)

        @pl.when(s == CHIPS)
        def _():
            @pl.loop(0, wt_s.shape[1] // HD)
            def _(j):
                wt_s[:, lanes_at(j, HD)] = w_s[lanes_at(j, HD), :].T

            pltpu.make_async_copy(wt_s, wt_out, wsem).start()
            rcopy(wt_s, wtp_out, wo_sem.at[TWO], wo_sem.at[TWO + ONE], p.partner).start()

    for n, (src, dst) in enumerate(whole):
        pltpu.make_async_copy(src, dst, osem.at[n]).wait()
    pltpu.make_async_copy(nall, nall, nall_sem).wait()
    pltpu.make_async_copy(wt_s, wt_out, wsem).wait()
    wo_copy.wait()
    rcopy(wt_s, wtp_out, wo_sem.at[TWO], wo_sem.at[TWO + ONE], p.partner).wait()
    for n, dev in enumerate(p.peers()):
        pos_copy(n, dev, dev).wait_send()
    ag_finish(p, *ag)


def attend_fwd_kernel(q, k, vt, posb, posr, wo, wop, x, gout, gain,
                      ot_out, lse_out, y_out, dproj_out, tail_out, dgain_out, *scratch):
    n_rs = len(rs_scratch(BLK))
    rs, rest = scratch[:n_rs], scratch[n_rs:]
    (q_s, k_s, vt_s, posb_s, wo_s, gain_s, x_s, go_s, o_s, ot_s, op_s, part, qt, s_buf, e_buf, l_buf, acc, yst, dgain, row_a,
     row_b, lsem, q_sem, op_ss, op_rs, osem, ysem, tail_sem) = rest
    fin, own = rs[HALF_PC], rs[HALF_PC + ONE]
    width = wo.shape[1]
    p = Place()
    loads = Loads(lsem)

    def q_load(s, flip):
        chip = lax.rem(p.chip + RS_OFF[s], CHIPS)
        g = (TWO * chip + lax.rem(p.core + flip, TWO)) * NBLK + RS_BLK[s]
        return pltpu.make_async_copy(q.at[:, g], q_s.at[:, g], q_sem.at[flip, s])

    first = [loads.add(k, k_s), loads.add(posb, posb_s), loads.add(vt, vt_s)]
    for flip in range(TWO):
        q_load(0, flip).start()
    e_buf[...] = jnp.zeros_like(e_buf)
    barrier((p.right, p.left, p.partner))
    wait_all(first + [q_load(0, flip) for flip in range(TWO)])
    second = [loads.add(wo, wo_s.at[pl.ds(0, QW)]), loads.add(wop, wo_s.at[pl.ds(QW, QW)])]
    for s in range(ONE, RS_STEPS):
        for flip in range(TWO):
            q_load(s, flip).start()

    def attend(pair, swap):
        walk = Walk(*pair)
        for n, g in enumerate(pair):
            qt[n] = q_s[:, g].reshape(TWO * BLK, HD).T
        acc[...] = jnp.zeros_like(acc)
        l_buf[...] = jnp.zeros_like(l_buf)

        def scores(i, a):
            n, _, t = walk.at(i)
            s_buf[a] = dot(k_s[t], qt[n])

        def values(i, a):
            n, _, t = walk.at(i)
            acc[n] += dot(vt_s[t], e_buf[a])

        def weights(i, a):
            n, g, t = walk.at(i)
            pos_q = walk.pos_q(i, posr[g])
            for c in range(KT // PIECE):
                keys = pl.ds(PIECE * c, PIECE)
                e = jnp.exp2(jnp.tanh(s_buf[a, keys, :] * (1.0 / SOFT_CAP)) * (SOFT_CAP * LOG2E))
                e = jnp.where(key_mask(pos_q, posb_s[t, keys, :]), e, 0.0)
                l_buf[n] += jnp.sum(e.reshape(PIECE // DEVS, DEVS, TWO * BLK), axis=0)
                e_buf[a, keys, :] = e.astype(BF16)

        def finish(n, g):
            l = jnp.sum(l_buf[n], axis=0, keepdims=True)
            lse_out[g] = jnp.log2(l)
            ot = acc[n] * (1.0 / l)
            for h in range(TWO):
                ot_s[h, :, lanes_at(g, BLK)] = ot[:, BLK * h:BLK * h + BLK].astype(BF16)
            o2 = ot.T.astype(BF16)
            for h in range(TWO):
                o_s[g, :, head(h)] = o2[BLK * h:BLK * h + BLK]

        scores(0, 0)

        @pl.loop(0, walk.turns)
        def _(turn):
            i = TWO * turn
            scores(i + ONE, ONE)
            values(i - ONE, ONE)
            weights(i, 0)
            scores(i + TWO, 0)
            values(i, 0)
            weights(i + ONE, ONE)

            @pl.when(lax.div(walk.na, TWO) == turn)
            def _():
                finish(0, walk.ga)
                swap.start()

        values(TWO * walk.turns - ONE, ONE)
        e_buf[...] = jnp.zeros_like(e_buf)
        finish(ONE, walk.gb)

    @pl.loop(0, RS_STEPS)
    def _(s):
        off, blk = pick(s, RS_OFF), pick(s, RS_BLK)
        chip = lax.rem(p.chip + off, CHIPS)
        mine = (TWO * chip + p.core) * NBLK + blk
        other = (TWO * chip + ONE - p.core) * NBLK + blk
        n = chip * NBLK + blk
        swap = rcopy(o_s.at[other], op_s.at[n], op_ss.at[n], op_rs.at[n], p.partner)
        attend((other, mine), swap)

        @pl.when(s == 0)
        def _():
            wait_all(second)
            wait_all([q_load(i, flip) for i in range(ONE, RS_STEPS) for flip in range(TWO)])

        swap.wait_recv()
        o_mine, o_part = o_s[mine], op_s[n]

        @pl.loop(0, TWO)
        def _(j):
            cols = lanes_at(j, width // TWO)
            part[:, cols] = dot(o_mine, wo_s[pl.ds(0, QW), cols]) + dot(o_part, wo_s[pl.ds(QW, QW), cols])

        rs_emit(p, s, part, *rs)

    third = [loads.add(x, x_s), loads.add(gout, go_s), loads.add(gain, gain_s.at[0])]
    outs = [pltpu.make_async_copy(ot_s, ot_out, osem)]
    outs[0].start()
    wait_all(third)
    dgain[...] = jnp.zeros_like(dgain)
    for blk in RS_DONE[:TWO]:
        rs_wait_block(p, blk, *rs)
        post_rows(functools.partial(rs_total, blk, fin, own), x_s.at[blk], go_s.at[blk], gain_s, yst.at[0, blk],
                  yst.at[ONE, blk], dgain, row_a, row_b)
        for n, dst in enumerate((y_out, dproj_out)):
            copy = pltpu.make_async_copy(yst.at[n, blk], dst.at[blk], ysem.at[n, blk])
            copy.start()
            outs.append(copy)
    dgain_out[...] = jnp.sum(dgain[...], axis=0, keepdims=True)
    blk = RS_DONE[TWO]
    rs_wait_block(p, blk, *rs)
    for h in range(TWO):
        srcs = (own.at[blk, half_of(h), :], fin.at[0, TWO * blk + h], fin.at[ONE, TWO * blk + h])
        for n, src in enumerate(srcs):
            copy = pltpu.make_async_copy(src, tail_out.at[n, h], tail_sem.at[n, h])
            copy.start()
            outs.append(copy)
    for n in range(MY_BLK):
        rcopy(op_s.at[n], op_s.at[n], op_ss.at[n], op_rs.at[n], p.partner).wait_send()
    rs_finish(p, *rs)
    wait_all(outs)


def attend_bwd_kernel(q_scale, dproj, tail, x, gout, gain, dgain_in, wo, q, k, kt, v, ot, lse, cos_t, sin_t, posb, posr,
                      dall, dqkv_out, y_out, dgain_out, *scratch):
    n_ag = len(ag_scratch(BLK))
    ag, rest = scratch[:n_ag], scratch[n_ag:]
    (tail_s, x_s, go_s, gain_s, y_s, dgain, row_a, row_b, wo_s, q_s, k_s, kt_s, v_s, ot_s, cos_s, sin_s, posb_s, dk_s, dv_s, dq_acc, out_s, qt, do_buf, dot_buf, delta, s_buf,
     dp_buf, p_buf, ds_buf, tail_sem, lsem, osem, own_sem, y_sem) = rest
    full = ag[0]
    p = Place()
    last = RS_DONE[TWO]
    early = Loads(tail_sem)
    inputs = [early.add(src, dst) for src, dst in ((tail, tail_s), (x.at[last], x_s), (gout.at[last], go_s),
                                                   (gain, gain_s.at[0]))]
    barrier((p.right, p.left, p.partner))

    def own_send(way, i):
        src = dproj.at[i // TWO, half_of(i), :] if i // TWO != last else piece_of(full, p.me, i)
        ag_send(p, way, i, src, *ag)

    def own_sends(late):
        for pieces in zip(*AG_FIRST):
            for way, i in enumerate(pieces):
                if (int(i) // TWO == last) == late:
                    own_send(way, int(i))

    own_sends(False)
    own = [pltpu.make_async_copy(dproj.at[b], full.at[p.me * NBLK + b], own_sem.at[b]) for b in RS_DONE[:TWO]]
    for b in RS_DONE[:TWO]:
        ag_swap(p, p.chip, b, dproj.at[b], full.at[p.me * NBLK + b], *ag).start()
    wait_all(inputs)
    arrays = ((wo, wo_s), (ot, ot_s), (q, q_s), (k, k_s), (kt, kt_s), (v, v_s), (posb, posb_s), (cos_t, cos_s),
              (sin_t, sin_s))
    loads = Loads(lsem)
    copies = [loads.add(src, dst) for src, dst in arrays]
    for copy in own:
        copy.start()
    dgain[...] = jnp.zeros_like(dgain)

    def tail_total(r, cols):
        per = PIECE // SUB
        h, rows = lax.div(r, per), rows16(lax.rem(r, per))
        total = tail_s[0, h, rows, cols].astype(F32)
        for n in (ONE, TWO):
            total = total + tail_s[n, h, rows, cols].astype(F32)
        return total.astype(BF16).astype(F32)

    g_last = p.me * NBLK + last
    post_rows(tail_total, x_s, go_s, gain_s, y_s, full.at[g_last], dgain, row_a, row_b)
    own_sends(True)
    ag_swap(p, p.chip, last, full.at[g_last], full.at[g_last], *ag).start()
    y_copy = pltpu.make_async_copy(y_s, y_out.at[0], y_sem)
    y_copy.start()
    dgain_out[...] = dgain_in[...] + jnp.sum(dgain[...], axis=0, keepdims=True)
    dk_s[...] = jnp.zeros_like(dk_s)
    dv_s[...] = jnp.zeros_like(dv_s)
    p_buf[...] = jnp.zeros_like(p_buf)
    ds_buf[...] = jnp.zeros_like(ds_buf)
    wait_all(own + copies + [y_copy])
    dq_cols, kv_cols = pl.ds(0, QW), pl.ds(QW, QW)

    @pl.loop(0, AG_STEPS)
    def _(s):
        pair = [ag_step(p, s, n, *ag) for n in range(TWO)]
        ag_then(s, own_send)
        walk = Walk(*pair)
        for g in pair:
            store_columns(full, dall, g, osem.at[0])
        rows = jnp.concatenate([full[g] for g in pair], axis=0)
        do_all = dot_bt(rows, wo_s[...]).astype(BF16)
        for n, g in enumerate(pair):
            do2 = heads_down(do_all[BLK * n:BLK * n + BLK])
            do_buf[n] = do2
            do_t = do2.T
            dot_buf[n] = do_t
            lanes = lanes_at(g, BLK)
            o_t = jnp.concatenate([ot_s[h, :, lanes] for h in range(TWO)], axis=1)
            delta[n] = jnp.sum(do_t.astype(F32) * o_t.astype(F32), axis=0, keepdims=True)
            qt[n] = q_s[:, g].reshape(TWO * BLK, HD).T
        dq_acc[...] = jnp.zeros_like(dq_acc)

        def scores(i, a):
            n, _, t = walk.at(i)
            s_buf[a] = dot(k_s[t], qt[n])
            dp_buf[a] = dot(v_s[t], dot_buf[n])

        def products(i, a):
            n, g, t = walk.at(i)
            dv_s[t] += dot(p_buf[a], do_buf[n])
            dk_s[t] += dot(ds_buf[a], q_s[:, g].reshape(TWO * BLK, HD))
            dq_acc[n] += dot(kt_s[t], ds_buf[a])

        def weights(i, a):
            n, g, t = walk.at(i)
            pos_q = walk.pos_q(i, posr[g])
            for c in range(KT // PIECE):
                keys = pl.ds(PIECE * c, PIECE)
                th = jnp.tanh(s_buf[a, keys, :] * (1.0 / SOFT_CAP))
                pr = jnp.exp2(th * (SOFT_CAP * LOG2E) - lse[g])
                pr = jnp.where(key_mask(pos_q, posb_s[t, keys, :]), pr, 0.0)
                p_buf[a, keys, :] = pr.astype(BF16)
                ds_buf[a, keys, :] = (pr * (dp_buf[a, keys, :] - delta[n]) * (1.0 - th * th)).astype(BF16)

        scores(0, 0)

        @pl.loop(0, walk.turns)
        def _(turn):
            i = TWO * turn
            scores(i + ONE, ONE)
            products(i - ONE, ONE)
            weights(i, 0)
            scores(i + TWO, 0)
            products(i, 0)
            weights(i + ONE, ONE)

            @pl.when(jnp.logical_and(s == AG_LAST - ONE, turn == jnp.minimum(TWO, walk.turns - ONE)))
            def _():
                ag_last(p, *ag)

        products(TWO * walk.turns - ONE, ONE)
        p_buf[...] = jnp.zeros_like(p_buf)
        ds_buf[...] = jnp.zeros_like(ds_buf)
        for n, g in enumerate(pair):
            dq = dq_acc[n].T
            for h in range(TWO):
                dq_h = rope_back(dq[BLK * h:BLK * h + BLK], cos_s[g], sin_s[g]) * q_scale
                out_s[g, :, head(h)] = dq_h.astype(BF16)
            pltpu.make_async_copy(out_s.at[g, :, dq_cols], dqkv_out.at[g, :, dq_cols], osem.at[ONE]).start()

    @pl.loop(0, ALL_BLK, unroll=CHIPS)
    def _(g):
        tile, rows = lax.div(g * BLK, KT), pl.ds(lax.rem(g, KT // BLK) * BLK, BLK)
        out_s[g, :, pl.ds(QW, HD)] = rope_back(dk_s[tile, rows, :], cos_s[g], sin_s[g]).astype(BF16)
        out_s[g, :, pl.ds(QW + HD, HD)] = dv_s[tile, rows, :].astype(BF16)
        pltpu.make_async_copy(out_s.at[g, :, kv_cols], dqkv_out.at[g, :, kv_cols], osem.at[TWO]).start()

    pltpu.make_async_copy(dall, dall, osem.at[0]).wait()
    pltpu.make_async_copy(out_s.at[:, :, dq_cols], dqkv_out.at[:, :, dq_cols], osem.at[ONE]).wait()
    pltpu.make_async_copy(out_s.at[:, :, kv_cols], dqkv_out.at[:, :, kv_cols], osem.at[TWO]).wait()
    ag_finish(p, *ag)


HOP_PLAN = ['O23', 'O01', 'O54', 'R54', 'L01', 'X01', 'X23', 'X45', 'R32', 'L23', 'R01', 'L54']
HOP_OFF, HOP_BLK = plan_tables(HOP_PLAN)
W_AHEAD = CHIPS
HOP_LATE = RS_STEPS - TWO
GROUPS = (digits('0145'), digits('23'))


def hop_emit(p, step, part, sent, turn, hop_l, hop_r, ss, hl_rs, hr_rs, result):
    kind = HOP_PLAN[step][0]
    for i in digits(HOP_PLAN[step][ONE:]):
        low, j = i < HALF_PC, i % HALF_PC
        hop, hop_rs, dev = (hop_l, hl_rs, p.right) if low else (hop_r, hr_rs, p.left)
        if kind == 'O':
            put_rows(part, sent.at[i], i)
            rcopy(sent.at[i], hop.at[j], ss.at[i], hop_rs.at[j], dev).start()
            continue
        n = 'RLX'.index(kind)
        if (kind == 'R' and low) or (kind == 'L' and not low):
            rcopy(hop.at[j], hop.at[j], ss.at[i], hop_rs.at[j], dev).wait_recv()
            put_rows(part, turn.at[n, i], i, hop.at[j])
        else:
            put_rows(part, turn.at[n, i], i)
        result(n, i).start()


def grad_rows_kernel(dqkv, wt, wtp, dg_post, *refs):
    n_out = TWO * len(GROUPS)
    hop_outs, (own_out, gpost_out), scratch = refs[:n_out], refs[n_out:n_out + TWO], refs[n_out + TWO:]
    (sent, turn, hop_l, hop_r, wt_s, d_s, dp_s, part, gains, ss, hl_rs, hr_rs, wt_sem, d_sem, dp_ss, dp_rs, out_sem, g_ss,
     g_rs, gsem) = scratch
    width = wt.shape[1]
    half, groups = width // TWO, width // QW
    p = Place()

    def w_loads(j):
        cols = lanes_at(j, QW)
        return [pltpu.make_async_copy(wt.at[:, cols], wt_s.at[pl.ds(0, QKV), cols], wt_sem.at[0, j]),
                pltpu.make_async_copy(wtp.at[:, cols], wt_s.at[pl.ds(QKV, QKV), cols], wt_sem.at[ONE, j])]

    def w_start(j):
        for copy in w_loads(j):
            copy.start()

    def block_of(off, blk, flip):
        chip = lax.rem(p.chip + off, CHIPS)
        return (TWO * chip + lax.rem(p.core + flip, TWO)) * NBLK + blk, chip * NBLK + blk

    def d_load(off, blk):
        g, n = block_of(off, blk, 0)
        return pltpu.make_async_copy(dqkv.at[g], d_s.at[n], d_sem.at[n])

    def d_swap(off, blk):
        other, n = block_of(off, blk, ONE)
        rcopy(dqkv.at[other], dp_s.at[n], dp_ss.at[n], dp_rs.at[n], p.partner).start()

    def result(n, i):
        dst = own_out.at[i]
        if n != TWO:
            group = [i in pieces for pieces in GROUPS].index(True)
            dst = hop_outs[n * len(GROUPS) + group].at[GROUPS[group].index(i)]
        return pltpu.make_async_copy(turn.at[n, i], dst, out_sem.at[n, i])

    plan = list(zip(HOP_OFF, HOP_BLK))
    d_load(*plan[0]).start()
    for j in range(W_AHEAD):
        w_start(j)
    barrier(p.peers())
    d_swap(*plan[0])
    send_gains(p, dg_post, gains, g_ss, g_rs)

    @pl.loop(0, RS_STEPS)
    def _(s):
        off, blk = pick(s, HOP_OFF), pick(s, HOP_BLK)
        _, n = block_of(off, blk, 0)
        late = jnp.where(s == HOP_LATE, I32(ONE), I32(0))
        d_load(off, blk).wait()
        rcopy(dp_s.at[n], dp_s.at[n], dp_ss.at[n], dp_rs.at[n], p.partner).wait_recv()
        d_mine, d_part = d_s[n], dp_s[n]

        def columns(cols):
            part[late, :, cols] = (dot(d_mine, wt_s[pl.ds(0, QKV), cols])
                                   + dot(d_part, wt_s[pl.ds(QKV, QKV), cols]))

        @pl.when(s == 0)
        def _():
            @pl.loop(0, groups)
            def _(j):
                @pl.when(j + W_AHEAD < groups)
                def _():
                    w_start(j + W_AHEAD)

                @pl.when(j + W_AHEAD == groups)
                def _():
                    for step in plan[ONE:]:
                        d_load(*step).start()
                        d_swap(*step)

                wait_all(w_loads(j))
                columns(lanes_at(j, QW))

        @pl.when(s != 0)
        def _():
            @pl.loop(0, TWO)
            def _(j):
                columns(lanes_at(j, half))

        @pl.when(s == RS_PLAN.index('X01'))
        def _():
            gain_total(p, dg_post, gains, gpost_out, g_ss, g_rs, gsem)

        for step in range(RS_STEPS):
            if step != HOP_LATE:
                @pl.when(s == step)
                def _(step=step):
                    if step > HOP_LATE:
                        hop_emit(p, HOP_LATE, part.at[ONE], sent, turn, hop_l, hop_r, ss, hl_rs, hr_rs, result)
                    hop_emit(p, step, part.at[0], sent, turn, hop_l, hop_r, ss, hl_rs, hr_rs, result)

    for i in range(NPC):
        rcopy(sent.at[i], sent.at[i], ss.at[i], hl_rs.at[0], p.right).wait_send()
    for n in range(MY_BLK):
        rcopy(dp_s.at[n], dp_s.at[n], dp_ss.at[n], dp_rs.at[n], p.partner).wait_send()
    for n in range(HALF_PC):
        for i in range(NPC):
            result(n, i).wait()


def gain_copy(n, src, gains, dev, owner, g_ss, g_rs):
    return rcopy(src, gains.at[owner], g_ss.at[n], g_rs.at[owner], dev)


def send_gains(p, src, gains, g_ss, g_rs):
    gains[p.me] = src[...]
    for n, dev in enumerate(p.peers()):
        gain_copy(n, src, gains, dev, p.me, g_ss, g_rs).start()


def gain_total(p, src, gains, out, g_ss, g_rs, gsem):
    for n, dev in enumerate(p.peers()):
        gain_copy(n, src, gains, dev, dev, g_ss, g_rs).wait()
    total = gains[0]
    for i in range(ONE, DEVS):
        total = total + gains[i]
    gains[p.me] = total
    copy = pltpu.make_async_copy(gains.at[p.me, 0], out, gsem)
    copy.start()
    copy.wait()


def weight_grads_kernel(dqkv, nall, dall, ot, y, y_last, gq_out, gk_out, gv_out, gwo_out, y_out, *scratch):
    d_s, in_s, gq_s, ot_s, gwo_s, y_s, lsem, isem, osem, wsem, ysem = scratch
    n_chunk = nall.shape[0]
    loads = Loads(lsem)
    first = loads.add(ot, ot_s)
    second = [loads.add(y_last.at[0], y_s.at[RS_DONE[TWO]])] + [loads.add(y.at[b], y_s.at[b]) for b in RS_DONE[:TWO]]
    d_copy = loads.add(dqkv, d_s)

    ahead = in_s.shape[0] - ONE

    def fetch(src, j, slot):
        pltpu.make_async_copy(src.at[j], in_s.at[slot], isem.at[slot]).start()

    def gwo_copies(j, slot):
        return [pltpu.make_async_copy(gwo_s.at[slot], gwo_out.at[:, lanes_at(j, HD)], wsem.at[slot])]

    def qkv_copies(j, slot):
        rows = lanes_at(j, HD)
        outs = (gq_out.at[rows, 0, :], gq_out.at[rows, ONE, :], gk_out.at[rows, 0, :], gv_out.at[rows, 0, :])
        return [pltpu.make_async_copy(gq_s.at[slot, :, head(n)], dst, osem.at[slot, n]) for n, dst in enumerate(outs)]

    def wo_chunk(a, slot):
        gwo_s[slot] = dot(ot_s[...], a)

    def qkv_chunk(a, slot):
        for h in range(TWO):
            cols = pl.ds(QW * h, QW)
            gq_s[slot, :, cols] = dot_at(a, d_s[:, :, cols].reshape(ALL_BLK * BLK, QW))

    def weight_grad(src, begun, after, compute, copies):
        @pl.loop(0, n_chunk)
        def _(j):
            at, slot = lax.rem(begun + j, ahead + ONE), lax.rem(j, TWO)
            pltpu.make_async_copy(src.at[j], in_s.at[at], isem.at[at]).wait()
            free = lax.rem(begun + j + ahead, ahead + ONE)

            @pl.when(j + ahead < n_chunk)
            def _():
                fetch(src, j + ahead, free)

            if after is not None:
                @pl.when(j + ahead >= n_chunk)
                def _():
                    fetch(after, j + ahead - n_chunk, free)

            @pl.when(j >= TWO)
            def _():
                wait_all(copies(j - TWO, slot))

            compute(in_s[at], slot)
            for copy in copies(j, slot):
                copy.start()

    for j in range(ahead):
        fetch(dall, j, j)
    first.wait()
    weight_grad(dall, 0, nall, wo_chunk, gwo_copies)
    d_copy.wait()
    wait_all(second)
    y_copy = pltpu.make_async_copy(y_s, y_out, ysem)
    y_copy.start()
    weight_grad(nall, n_chunk, None, qkv_chunk, qkv_copies)
    for j in (n_chunk - TWO, n_chunk - ONE):
        wait_all(gwo_copies(j, j % TWO) + qkv_copies(j, j % TWO))
    y_copy.wait()


def pre_load(pieces, from_left, from_right, own, x, gout, blocks, lsem):
    copies = []
    for m, i in enumerate(pieces):
        srcs = (from_left.at[m], from_right.at[m], own.at[i], x.at[i], gout.at[i])
        copies.append([pltpu.make_async_copy(src, blocks.at[n, m], lsem.at[n, m]) for n, src in enumerate(srcs)])
        for copy in copies[m]:
            copy.start()
    return copies


def pre_sums(blocks, m, gain, dn_s, stat, dgain):
    from_left, from_right, own, x, _ = (blocks.at[n, m] for n in range(blocks.shape[0]))
    width = x.shape[1]

    @pl.loop(0, PIECE // SUB)
    def _(r):
        rows, sums, dots = rows16(r), [], []
        for cols in column_groups(width):
            val = x[rows, cols].astype(F32)
            dn = (own[rows, cols].astype(F32) + from_left[rows, cols].astype(F32)
                  + from_right[rows, cols].astype(F32)).astype(BF16).astype(F32)
            dn_s[m, rows, cols] = dn
            sums.append(fold(val * val))
            dots.append(fold(dn * (1.0 + gain[:, cols]) * val))
        inv = lax.rsqrt(row_mean(sums, width) + NORM_EPS)
        stat[0, m, rows, :] = jnp.broadcast_to(inv, (SUB, HD2))
        stat[ONE, m, rows, :] = jnp.broadcast_to(row_mean(dots, width) * inv, (SUB, HD2))
        for cols in column_groups(width):
            dg = dn_s[m, rows, cols] * (x[rows, cols].astype(F32) * inv)
            dgain[:, cols] += dg[:DEVS] + dg[DEVS:]


def pre_result(blocks, m, gain, dn_s, stat, gx):
    x, gout = blocks.at[NBLK, m], blocks.at[NBLK + ONE, m]

    @pl.loop(0, PIECE // SUB)
    def _(r):
        rows = rows16(r)
        inv, mean = stat[0, m, rows, 0:1], stat[ONE, m, rows, 0:1]
        for cols in column_groups(x.shape[1]):
            nrm = x[rows, cols].astype(F32) * inv
            dx = (inv * (dn_s[m, rows, cols] * (1.0 + gain[:, cols]) - nrm * mean)).astype(BF16).astype(F32)
            gx[m, rows, cols] = (gout[rows, cols].astype(F32) + dx).astype(BF16)


def pre_grad_kernel(pieces, from_left, from_right, own, x, gout, gain, gx_out, dgain, blocks, gain_s, dn_s, stat, gx, lsem,
                    xsem, gsem):
    copies = pre_load(pieces, from_left, from_right, own, x, gout, blocks, lsem)
    gain_in = pltpu.make_async_copy(gain, gain_s.at[0], gsem)
    gain_in.start()
    dgain[...] = jnp.zeros_like(dgain)
    gain_in.wait()
    for m, i in enumerate(pieces):
        wait_all(copies[m])
        pre_sums(blocks, m, gain_s, dn_s, stat, dgain)
        pre_result(blocks, m, gain_s, dn_s, stat, gx)
        pltpu.make_async_copy(gx.at[m], gx_out.at[i], xsem.at[m]).start()
    for m, i in enumerate(pieces):
        pltpu.make_async_copy(gx.at[m], gx_out.at[i], xsem.at[m]).wait()


def pre_scratch(n, width):
    return [pltpu.VMEM((NBLK + TWO, n, PIECE, width), BF16), pltpu.VMEM((ONE, width), F32),
            pltpu.VMEM((n, PIECE, width), F32), pltpu.VMEM((TWO, n, PIECE, HD2), F32), pltpu.VMEM((n, PIECE, width), BF16),
            pltpu.SemaphoreType.DMA((NBLK + TWO, n))]


def pre_grad(pieces, *args):
    x, dma = args[NBLK], pltpu.SemaphoreType.DMA
    width = x.shape[TWO]
    return pl.pallas_call(
        functools.partial(pre_grad_kernel, pieces), name='pre_grad',
        out_shape=(sds(x.shape, BF16), sds((DEVS, width), F32)), in_specs=specs('AAAAAA'), out_specs=specs('AV'),
        scratch_shapes=pre_scratch(len(pieces), width) + [dma((len(pieces),)), dma(())],
        compiler_params=pltpu.CompilerParams(vmem_limit_bytes=VMEM_BYTES))(*args)


def last_rows_kernel(from_left, from_right, own, x, gout, gain, dgain_in, gx_out, gpre_out, *scratch):
    blocks, gain_s, dn_s, stat, gx, psem, dgain, row, gains, lsem, xsem, g_ss, g_rs, gsem = scratch
    pieces = GROUPS[ONE]
    p = Place()
    copies = pre_load(pieces, from_left, from_right, own, x, gout, blocks, psem)
    loads = Loads(lsem)
    rest = [loads.add(gain, gain_s.at[0]), loads.add(dgain_in, dgain)]
    barrier(p.peers())
    wait_all(rest)
    for m in range(len(pieces)):
        wait_all(copies[m])
        pre_sums(blocks, m, gain_s, dn_s, stat, dgain)
    row[...] = jnp.sum(dgain[...], axis=0, keepdims=True)
    send_gains(p, row, gains, g_ss, g_rs)
    for m in range(len(pieces)):
        pre_result(blocks, m, gain_s, dn_s, stat, gx)
    result = pltpu.make_async_copy(gx, gx_out, xsem)
    result.start()
    gain_total(p, row, gains, gpre_out, g_ss, g_rs, gsem)
    result.wait()


def finish_kernel(gx_last, gpre, gpost, gx_in, gx_out, gpre_out, gpost_out, blk_s, pre_s, post_s, get, put):
    moves = ((gx_last, blk_s, gx_out.at[pl.ds(GROUPS[ONE][0], len(GROUPS[ONE]))]), (gpre, pre_s, gpre_out), (gpost, post_s, gpost_out))
    for n, (src, buf, dst) in enumerate(moves):
        pltpu.make_async_copy(src, buf, get.at[n]).start()
    for n, (src, buf, dst) in enumerate(moves):
        pltpu.make_async_copy(src, buf, get.at[n]).wait()
        pltpu.make_async_copy(buf, dst, put.at[n]).start()
    for n, (src, buf, dst) in enumerate(moves):
        pltpu.make_async_copy(buf, dst, put.at[n]).wait()


def specs(places):
    return [pl.BlockSpec(memory_space={'A': pl.ANY, 'V': pltpu.VMEM}[place]) for place in places]


def params(cid):
    return pltpu.CompilerParams(collective_id=cid, has_side_effects=True, vmem_limit_bytes=VMEM_BYTES)


def sds(shape, dtype):
    return jax.ShapeDtypeStruct(shape, dtype)


def solution(mesh):
    act_spec = P('dp', 'tp', None)
    head_spec = P(None, 'tp', None)
    grad_spec = P('dp', 'tp', None)
    in_specs = (act_spec, P('dp', 'tp'), act_spec, head_spec, head_spec, head_spec, P('tp', None, None), P(None), P(None))
    out_specs = (act_spec, act_spec, grad_spec, grad_spec, grad_spec, P(('dp', 'tp'), None, None), P('dp'), P('dp'))
    assert mesh.shape['tp'] == DEVS

    def local_step(x_in, positions, grad_out, w_query, w_key, w_value, w_out, gain_pre, gain_post):
        width, _, head_dim = w_query.shape
        q_scale = head_dim ** -0.5
        rows = ALL_BLK * BLK
        tiles = rows // KT
        dma = pltpu.SemaphoreType.DMA
        vm = pltpu.VMEM
        x_blk = x_in.reshape(NBLK, BLK, width)
        go_blk = grad_out.reshape(NBLK, BLK, width)
        wo = w_out.reshape(QW, width)
        inv_freq = (ROPE_THETA ** (-2.0 * np.arange(HD2) / head_dim)).astype(np.float32).reshape(ONE, HD2)

        all_bf, rope_t = sds((width // HD, ALL_BLK, BLK, HD), BF16), sds((ALL_BLK, BLK, HD2), F32)
        blocks, tiles_t = sds((ALL_BLK, BLK, HD), BF16), sds((tiles, HD, KT), BF16)
        pos_blk, pos_row = sds((ALL_BLK, BLK, HD2), I32), sds((ALL_BLK, ONE, HD2), I32)
        q_all, w_t, own_rows = sds((TWO, ALL_BLK, BLK, HD), BF16), sds((QKV, width), BF16), sds(x_blk.shape, BF16)
        o_all, ot_all, lse_all = sds((ALL_BLK, BLK, QW), BF16), sds((TWO, HD, rows), BF16), sds((ALL_BLK, ONE, HD), F32)
        d_all, gain_row = sds((ALL_BLK, BLK, QKV), BF16), sds((ONE, width), F32)

        def like(*specs):
            return [vm(spec.shape, spec.dtype) for spec in specs]

        (nall, q, k, v, kt, vt, cos_t, sin_t, posb, posr, wt, wtp, wop) = pl.pallas_call(
            functools.partial(gather_qkv_kernel, q_scale), name='gather_qkv',
            out_shape=(all_bf, q_all, blocks, blocks, tiles_t, tiles_t, rope_t, rope_t, pos_blk, pos_row, w_t, w_t,
                       sds(wo.shape, BF16)),
            in_specs=specs('AVVAAAAA'), out_specs=specs('AAAAAAAAAVAAA'),
            scratch_shapes=ag_scratch(width) + like(
                own_rows, gain_row, sds(w_query.shape, BF16), sds((width, QKV), BF16), w_t, q_all, blocks, blocks, tiles_t, tiles_t, rope_t, rope_t,
                pos_blk, pos_row) + [dma((10,)), dma((9,)), dma(()), dma((CHIPS,)), dma((DEVS,)), dma((DEVS,)), dma(())],
            compiler_params=params(0),
        )(x_blk, positions.reshape(NBLK, ONE, BLK), inv_freq, gain_pre, w_query, w_key.reshape(width, HD), w_value.reshape(width, HD), wo)

        k_t, v_t, posb_t = (a.reshape(tiles, KT, a.shape[2]) for a in (k, v, posb))
        tile_rows, tile_f = sds(k_t.shape, BF16), sds(k_t.shape, F32)
        tile_pos, score, square = sds(posb_t.shape, I32), sds((TWO, KT, HD), F32), sds((TWO, HD, HD), BF16)
        square_f, part = sds((TWO, HD, HD), F32), sds((BLK, width), F32)
        tail_all, row_block = sds((NBLK, TWO, PIECE, width), BF16), sds((BLK, width), BF16)
        ot, lse, y, dproj, tail, dg_post = pl.pallas_call(
            attend_fwd_kernel, name='attend_fwd',
            out_shape=(ot_all, lse_all, own_rows, own_rows, tail_all, gain_row),
            in_specs=specs('AAAAVAAAAA'), out_specs=specs('AVAAAV'),
            scratch_shapes=rs_scratch(width) + like(
                q_all, tile_rows, tiles_t, tile_pos, w_t, gain_row, own_rows, own_rows, o_all, ot_all,
                sds((MY_BLK, BLK, QW), BF16), part, square, score, sds(score.shape, BF16), sds((TWO, DEVS, HD), F32),
                square_f, sds((TWO,) + x_blk.shape, BF16), sds((DEVS, width), F32), sds((SUB, width), F32),
                sds((SUB, width), F32))
            + [dma((8,)), dma((TWO, RS_STEPS)), dma((MY_BLK,)), dma((MY_BLK,)), dma(()), dma((TWO, NBLK)), dma((NBLK, TWO))],
            compiler_params=params(1),
        )(q, k_t, vt, posb_t, posr, wo, wop, x_blk, go_blk, gain_post)

        dall, dqkv, y_last, dg_post = pl.pallas_call(
            functools.partial(attend_bwd_kernel, q_scale), name='attend_bwd',
            out_shape=(all_bf, d_all, sds((ONE, BLK, width), BF16), gain_row),
            in_specs=specs('AAAAAVAAAAAAVAAAV'), out_specs=specs('AAAV'),
            scratch_shapes=ag_scratch(width) + like(
                tail_all, row_block, row_block, gain_row, row_block, sds((DEVS, width), F32), sds((SUB, width), F32),
                sds((SUB, width), F32), sds(wo.shape, BF16), q_all, tile_rows, tiles_t, tile_rows, ot_all, rope_t, rope_t, tile_pos, tile_f, tile_f,
                square_f, d_all, square, square, square, sds((TWO, ONE, HD), F32), score, score, sds(score.shape, BF16),
                sds(score.shape, BF16))
            + [dma((4,)), dma((9,)), dma((3,)), dma((NBLK,)), dma(())],
            compiler_params=params(2),
        )(dproj, tail, x_blk, go_blk, gain_post, dg_post, wo, q, k_t, kt, v_t, ot, lse, cos_t, sin_t, posb_t, posr)

        hops = [sds((len(pieces), PIECE, width), BF16) for pieces in GROUPS]
        piece, own_pieces = sds((HALF_PC, PIECE, width), BF16), sds((NPC, PIECE, width), BF16)
        gain_all, d_mine = sds((DEVS, ONE, width), F32), sds((MY_BLK, BLK, QKV), BF16)
        *to_all, own, gpost = pl.pallas_call(
            grad_rows_kernel, name='grad_rows',
            out_shape=hops + hops + [own_pieces, sds((width,), F32)],
            in_specs=specs('AAAV'), out_specs=specs('AAAAAA'),
            scratch_shapes=like(
                own_pieces, sds((HALF_PC, NPC, PIECE, width), BF16), piece, piece,
                sds((TWO * QKV, width), BF16), d_mine, d_mine, sds((TWO, BLK, width), F32), gain_all)
            + [dma((NPC,)), dma((HALF_PC,)), dma((HALF_PC,)), dma((TWO, width // QW)), dma((MY_BLK,)),
               dma((MY_BLK,)), dma((MY_BLK,)), dma((HALF_PC, NPC)), dma((DEVS,)), dma((DEVS,)), dma(())],
            compiler_params=params(3),
        )(dqkv, wt, wtp, dg_post)

        def shift(rows_out, way):
            ring = [(TWO * c + k, TWO * ((c + way) % CHIPS) + k) for c in range(CHIPS) for k in range(TWO)]
            return lax.ppermute(rows_out, 'tp', ring)

        hops_in = []
        for n in range(len(GROUPS)):
            hops_in.append((shift(to_all[n], ONE), shift(to_all[n + len(GROUPS)], CHIPS - ONE)))
        flops = TWO * rows * width * (QKV + QW)
        gq, gk, gv, gwo, y = pl.pallas_call(
            weight_grads_kernel, name='weight_grads',
            out_shape=(sds(w_query.shape, F32), sds(w_key.shape, F32), sds(w_value.shape, F32), sds(wo.shape, F32),
                       own_rows),
            in_specs=specs('AAAAAA'), out_specs=specs('AAAAA'),
            scratch_shapes=like(
                d_all, sds((CHIPS, rows, HD), BF16), sds((TWO, HD, QKV), F32), sds((QW, rows), BF16), sds((TWO, QW, HD), F32),
                own_rows) + [dma((5,)), dma((CHIPS,)), dma((TWO, CHIPS)), dma((TWO,)), dma(())],
            cost_estimate=pl.CostEstimate(flops=flops, bytes_accessed=TWO * rows * width * CHIPS, transcendentals=0),
            compiler_params=pltpu.CompilerParams(vmem_limit_bytes=VMEM_BYTES),
        )(dqkv, *(a.reshape(width // HD, rows, HD) for a in (nall, dall)), ot.reshape(QW, rows), y,
          y_last)
        x_pc, go_pc = x_in.reshape(NPC, PIECE, width), grad_out.reshape(NPC, PIECE, width)
        gx, dgain = pre_grad(GROUPS[0], *hops_in[0], own, x_pc, go_pc, gain_pre)
        block = hops[ONE]
        gx_last, gpre = pl.pallas_call(
            last_rows_kernel, name='last_rows', out_shape=(block, sds((width,), F32)),
            in_specs=specs('AAAAAAA'), out_specs=specs('AA'),
            scratch_shapes=pre_scratch(block.shape[0], width) + like(sds((DEVS, width), F32), gain_row, gain_all)
            + [dma((TWO,)), dma(()), dma((DEVS,)), dma((DEVS,)), dma(())],
            compiler_params=params(4),
        )(*hops_in[ONE], own, x_pc, go_pc, gain_pre, dgain)
        gx, gpre, gpost = pl.pallas_call(
            finish_kernel, name='finish', out_shape=(own_pieces, sds((width,), F32), sds((width,), F32)),
            in_specs=specs('AAAA'), out_specs=specs('AAA'), input_output_aliases={3: 0},
            scratch_shapes=like(block, sds((width,), F32), sds((width,), F32)) + [dma((3,)), dma((3,))],
            compiler_params=pltpu.CompilerParams(vmem_limit_bytes=VMEM_BYTES),
        )(gx_last, gpre, gpost, gx)
        return (y.reshape(x_in.shape), gx.reshape(x_in.shape), gq, gk, gv, gwo.reshape(w_out.shape), gpre, gpost)

    return jax.shard_map(local_step, mesh=mesh, in_specs=in_specs, out_specs=out_specs, check_vma=False)
```
